32 devices in a mesh: dp: 2 (over x), seq: 16 (over z, y, core).
Axes of the slice: x: 2, y: 2, z: 4, core: 2. Of those that a mesh axis runs over, the one named last changes fastest.
Arguments:
- tiles: bfloat16 [2, 16, 32, 4, 1024], P('dp', None, 'seq'), may hold values from -6 to 6
- patch_index: int32 [2, 16, 32, 4], P('dp', None, 'seq'), may hold values from 0 to 127
- pos_table: bfloat16 [128, 1024], replicated, may hold values from -6 to 6
- depth_kernel: bfloat16 [2, 27, 1024], replicated, may hold values from -1.25 to 1.25
- enc_gain: bfloat16 [2, 1024], replicated, may hold values from 0.099609375 to 1.8984375
- point_weight: bfloat16 [2, 1024, 1024], replicated, may hold values from -0.1875 to 0.1875
- action_ids: int32 [2, 16], replicated, may hold values from 0 to 7
- w_in: bfloat16 [1024, 5120], P('seq', 'dp'), may hold values from -0.1875 to 0.1875
- action_table: bfloat16 [8, 5120], P(None, 'dp'), may hold values from -6 to 6
- dyn_gain: bfloat16 [5120], P('dp'), may hold values from 0.099609375 to 1.8984375
- w_query: bfloat16 [5120, 5120], P('seq', 'dp'), may hold values from -0.078125 to 0.078125
- w_keyval: bfloat16 [5120, 2, 1024], P('seq', None, 'dp'), may hold values from -0.078125 to 0.078125
- seq_order: int32 [4], replicated, may hold values from 0 to 3, each once
Outputs:
- attended: bfloat16 [2, 16, 32, 4, 5120], P(None, None, 'seq', None, 'dp')
The draws below stay inside these ranges and needn't reach their ends.
Inputs may be any that keep to these rules, and one draw needn't show every extreme that they name: `seq_order`: each of 0 to 3 appears once.
All inputs are finite; a program needn't handle non-finite values.
Results may differ from the reference program's by a relative error of at most 0.012.
Values may be sent and summed in bfloat16 or wider, within the bound.
A program may use at most 128 MiB of HBM per device.

```python
import jax
import jax.numpy as jnp
from jax import lax

ENC = 1024
DIM = 5120
HEAD = 128
Q_HEADS = 40
KV_HEADS = 8
ACTIONS = 8
FRAMES = 16
LAYERS = 2
COLS = 4
CLIPS = 2
ROWS = 32
POSITIONS = 128


def with_ends(values, key, low, top_value):
    dims = values.shape
    spot = [jax.random.randint(jax.random.fold_in(key, axis), (), 0, dims[axis]) for axis in range(len(dims))]
    values = values.at[tuple(spot)].set(low)
    longest = dims.index(max(dims))
    spot[longest] = (spot[longest] + 1) % dims[longest]
    return values.at[tuple(spot)].set(top_value)


def steps_of(stream_key, shape, split, least, high):
    factor_of, own = 1.0, jax.random.fold_in(stream_key, 6)
    for dim, blocks in split:
        draws = jnp.exp(jax.random.uniform(jax.random.fold_in(own, dim), (blocks,), jnp.float32, least / len(split), high / len(split)))
        factor_of = factor_of * jnp.repeat(draws, shape[dim] // blocks).reshape([-1 if axis == dim else 1 for axis in range(len(shape))])
    return factor_of


def scatter_about(stream_key, dims, width, limit, shards=(), kind=jnp.bfloat16):
    entries = width * jax.random.normal(stream_key, dims, jnp.float32)
    if shards:
        entries = entries * steps_of(stream_key, dims, shards, -0.22, 0.18)
    return jnp.clip(entries, -limit, limit).astype(kind)


def setup_inputs(seed: int = 0) -> dict:
    arg_keys = jax.random.split(jax.random.key(seed), 14)
    return {
        "tiles": scatter_about(arg_keys[0], (CLIPS, FRAMES, ROWS, COLS, ENC), 1.0, 6.0, ((0, 2), (2, 16))),
        "patch_index": with_ends(jax.random.randint(arg_keys[1], (CLIPS, FRAMES, ROWS, COLS), 0, POSITIONS), jax.random.fold_in(arg_keys[1], 1), 0, POSITIONS - 1).astype(jnp.int32),
        "pos_table": scatter_about(arg_keys[2], (POSITIONS, ENC), 1.0, 6.0),
        "depth_kernel": scatter_about(arg_keys[3], (LAYERS, 27, ENC), 27 ** -0.5, 1.25),
        "enc_gain": jnp.clip(1.0 + 0.18 * jax.random.normal(arg_keys[4], (LAYERS, ENC), jnp.float32), 0.099609375, 1.8984375).astype(jnp.bfloat16),
        "point_weight": scatter_about(arg_keys[5], (LAYERS, ENC, ENC), ENC ** -0.5, 0.1875),
        "action_ids": with_ends(jax.random.randint(arg_keys[6], (CLIPS, FRAMES), 0, ACTIONS), jax.random.fold_in(arg_keys[6], 1), 0, ACTIONS - 1).astype(jnp.int32),
        "w_in": scatter_about(arg_keys[7], (ENC, DIM), ENC ** -0.5, 0.1875, ((0, 16), (1, 2))),
        "action_table": scatter_about(arg_keys[8], (ACTIONS, DIM), 1.0, 6.0, ((1, 2),)),
        "dyn_gain": jnp.clip(1.0 + 0.18 * jax.random.normal(arg_keys[9], (DIM,), jnp.float32), 0.099609375, 1.8984375).astype(jnp.bfloat16),
        "w_query": scatter_about(arg_keys[10], (DIM, DIM), DIM ** -0.5, 0.078125, ((0, 16), (1, 2))),
        "w_keyval": scatter_about(arg_keys[11], (DIM, 2, KV_HEADS * HEAD), DIM ** -0.5, 0.078125, ((0, 16), (2, 2))),
        "seq_order": jax.random.permutation(arg_keys[12], COLS).astype(jnp.int32),
    }


def depth_block(padded, kernel, gains, weight):
    frames = padded.shape[1]
    height = padded.shape[2] - 2
    breadth = padded.shape[3]
    channels = padded.shape[4]
    framed = jnp.pad(padded.astype(jnp.float32), ((0, 0), (2, 0), (0, 0), (1, 1), (0, 0)))
    summed = jnp.zeros((padded.shape[0], frames, height, breadth, channels), jnp.float32)
    for time_tap in range(3):
        for row_tap in range(3):
            for col_tap in range(3):
                window = framed[:, time_tap:time_tap + frames, row_tap:row_tap + height, col_tap:col_tap + breadth, :]
                summed = summed + window * kernel[9 * time_tap + 3 * row_tap + col_tap].astype(jnp.float32)
    factor = lax.rsqrt(lax.optimization_barrier(jnp.mean(summed * summed, axis=-1, keepdims=True)) + 1e-05)
    normed = (summed * factor * gains.astype(jnp.float32)).astype(jnp.bfloat16)
    projected = jnp.dot(normed.reshape(-1, channels), weight, preferred_element_type=jnp.float32).reshape(summed.shape)
    centre = padded[:, :, 1:-1].astype(jnp.float32)
    return (centre + jax.nn.gelu(projected)).astype(jnp.bfloat16)

def temporal_mix(query_heads, key_heads, value_heads):
    frames = query_heads.shape[1]
    query_unit = query_heads * lax.rsqrt(lax.optimization_barrier(jnp.mean(query_heads * query_heads, axis=-1, keepdims=True)) + 1e-06)
    key_unit = key_heads * lax.rsqrt(lax.optimization_barrier(jnp.mean(key_heads * key_heads, axis=-1, keepdims=True)) + 1e-06)
    scores = jnp.einsum('cfpkgh,ctpkh->cpkgft', query_unit, key_unit, precision=lax.Precision.HIGHEST) * HEAD ** (-0.5)
    causal = jnp.arange(frames, dtype=jnp.int32)[:, None] >= jnp.arange(frames, dtype=jnp.int32)[None, :]
    raised = jnp.where(causal, jnp.exp(scores), 0.0)
    shares = (raised / lax.optimization_barrier(jnp.sum(raised, axis=-1, keepdims=True))).astype(jnp.bfloat16)
    mixed = jnp.einsum('cpkgft,ctpkh->cfpkgh', shares.astype(jnp.float32), value_heads.astype(jnp.float32), precision=lax.Precision.HIGHEST)
    return mixed.astype(jnp.bfloat16)

def reference(tiles, patch_index, pos_table, depth_kernel, enc_gain, point_weight, action_ids, w_in, action_table, dyn_gain, w_query, w_keyval, seq_order):
    placed = jnp.take(pos_table, patch_index, axis=0).astype(jnp.float32)
    hidden = (tiles.astype(jnp.float32) + placed).astype(jnp.bfloat16)
    for block_idx in range(LAYERS):
        padded = jnp.pad(hidden, ((0, 0), (0, 0), (1, 1), (0, 0), (0, 0)))
        hidden = depth_block(padded, depth_kernel[block_idx], enc_gain[block_idx], point_weight[block_idx])
    group = Q_HEADS // KV_HEADS
    cells = ROWS * COLS

    def one_clip(inputs_pair):
        latent, frame_ids = inputs_pair
        embed = jnp.dot(latent.reshape(-1, ENC), w_in, preferred_element_type=jnp.float32).reshape(FRAMES, cells, DIM)
        embed = embed + jnp.take(action_table, frame_ids, axis=0).astype(jnp.float32)[:, None, :]
        embed = jax.nn.gelu(embed)
        factor = lax.rsqrt(lax.optimization_barrier(jnp.mean(embed * embed, axis=-1, keepdims=True)) + 1e-05)
        normed = (embed * factor * dyn_gain.astype(jnp.float32)).astype(jnp.bfloat16).reshape(-1, DIM)
        query = jnp.dot(normed, w_query, preferred_element_type=jnp.float32)
        keyval = jnp.dot(normed, w_keyval.reshape(DIM, -1), preferred_element_type=jnp.float32)
        query_heads = query.reshape(1, FRAMES, cells, KV_HEADS, group, HEAD)
        pairs = keyval.reshape(1, FRAMES, cells, 2, KV_HEADS, HEAD)
        mixed = temporal_mix(query_heads, pairs[:, :, :, 0], pairs[:, :, :, 1].astype(jnp.bfloat16))
        return mixed.reshape(FRAMES, ROWS, COLS, DIM)
    mixed_all = lax.map(one_clip, (hidden, action_ids))
    return jnp.take(mixed_all, seq_order, axis=3)
```

```python
import functools
import math

import jax
import jax.numpy as jnp
from jax import lax
from jax.experimental import pallas as pl
from jax.experimental.pallas import tpu as pltpu
from jax.sharding import PartitionSpec as P

DIM = 5120
HEAD = 128
Q_HEADS = 40
KV_HEADS = 8
MESH = pl.DeviceIdType.MESH


def gelu(z):
    return 0.5 * z * (1.0 + jnp.tanh(0.7978845608028654 * (z + 0.044715 * (z * z * z))))


def flipped(t, mask, bits):
    for bit in bits:
        if mask & bit:
            t = t + bit - 2 * bit * ((t // bit) % 2)
    return t


def window_kernel(
    sizes,
    pack_ref,
    in_ref,
    aux_ref,
    start_ref,
    taps_ref,
    gains_ref,
    point_ref,
    pick_ref,
    out_ref,
    w_all,
    in_all,
    aux_all,
    lat_all,
    embeds,
    squares,
    mixed,
    keys,
    values,
    halos,
    middle,
    conv,
    latent_ref,
    h_send,
    h_recv,
    w_send,
    w_recv,
    i_send,
    i_recv,
    l_send,
    l_recv,
    a_send,
    a_recv,
    o_send,
    o_recv,
    own_sem,
    zi_send,
    zl_send,
):
    D, C, T, edge = sizes
    d = lax.axis_index("dp")
    seq = lax.axis_index("seq")
    c = seq // T
    t = seq % T
    bits = []
    bit = T // 2
    while bit:
        bits.append(bit)
        bit //= 2
    early, last = bits[:-1], bits[-1]
    near_masks = [m for m in range(T) if not m & last]
    near_masks.sort(key=lambda m: m.bit_count())
    depth = pack_ref.shape[1]
    in_rows, in_cols = in_ref.shape
    tokens = latent_ref.shape[0]
    group = Q_HEADS // KV_HEADS
    qcols = group * HEAD

    orders = [
        sorted(range(C), key=lambda o, i=i: (abs(o - i), o if 2 * i < C else -o)) for i in range(C)
    ]

    def nearest(h):
        value = orders[0][h]
        for i in range(1, C):
            value = jnp.where(c == i, orders[i][h], value)
        return value

    origins = [c] + [nearest(h) for h in range(1, C)]

    def to_c(shift):
        return (d, ((c + shift) % C) * T + t)

    def to_t(bit):
        return (d, c * T + flipped(t, bit, bits))

    def to_d(shift):
        return ((d + shift) % D, seq)

    peers = [to_c(s) for s in range(1, C)] + [to_t(b) for b in bits] + [to_d(s) for s in range(1, D)]
    S = C * T
    above, below = (d, (seq + S - 1) % S), (d, (seq + 1) % S)
    peers += [above, below]
    with jax.named_scope("barrier"):
        barrier = pltpu.get_barrier_semaphore()
        for peer in peers:
            pl.semaphore_signal(barrier, inc=1, device_id=peer, device_id_type=MESH)
        pl.semaphore_wait(barrier, len(peers))

    sends = []

    def push(src, dst, send_sem, recv_sem, peer, guard=None):
        copy = pltpu.make_async_remote_copy(
            src_ref=src,
            dst_ref=dst,
            send_sem=send_sem,
            recv_sem=recv_sem,
            device_id=peer,
            device_id_type=MESH,
        )
        if guard is None:
            copy.start()
        else:
            pl.when(guard)(copy.start)
        sends.append((copy, guard))

    def arrived(ref, sem):
        pltpu.make_async_copy(ref, ref, sem).wait()

    w_cols = ((0, edge), (edge, pack_ref.shape[2] - edge))
    pieces = [(g, r) for g in range(2) for r in range(2)]

    def w_slot(o, m, piece):
        g, r = piece
        origin = o * T + flipped(t, m, bits)
        return w_all.at[
            pl.ds(pl.multiple_of(origin * depth + r * (depth // 2), depth // 2), depth // 2),
            pl.ds(*w_cols[g]),
        ]

    def w_own(target, piece):
        g, r = piece
        return pack_ref.at[target, pl.ds(r * (depth // 2), depth // 2), pl.ds(*w_cols[g])]

    split = in_rows * 3 // 4
    WHOLE, HEAD_PART, TAIL_PART = 0, 1, 2

    def part_rows(part):
        return ((0, in_rows), (0, split), (split, in_rows - split))[part]

    def i_slot(o, m, e, part):
        first, count = part_rows(part)
        origin = o * T + flipped(t, m, bits)
        column = ((d + D - e) % D) * in_cols
        return in_all.at[
            pl.ds(pl.multiple_of(origin * in_rows + first, math.gcd(in_rows, split)), count),
            pl.ds(pl.multiple_of(column, HEAD), in_cols),
        ]

    def l_slot(o, e):
        row = ((d + D - e) % D) * tokens
        return lat_all.at[o, pl.ds(pl.multiple_of(row, tokens), tokens)]

    def a_slot(e):
        column = ((d + D - e) % D) * in_cols
        return aux_all.at[:, pl.ds(pl.multiple_of(column, HEAD), in_cols)]

    def along(o):
        ahead = jnp.where(o < c, 1, -1)
        target = c + ahead
        guard = (target >= 0) & (target < C)
        return (d, jnp.clip(target, 0, C - 1) * T + t), guard

    def below_above(src, dst, send_sems, recv_sem):
        if C == 1:
            return
        push(src, dst, send_sems.at[0], recv_sem, (d, jnp.minimum(c + 1, C - 1) * T + t), c + 1 < C)
        push(src, dst, send_sems.at[1], recv_sem, (d, jnp.maximum(c - 1, 0) * T + t), c >= 1)

    def w_forward(o, m, piece, src):
        k = pieces.index(piece)
        low = -1
        for b in bits:
            if m & b:
                low = bits.index(b)
        for b in bits[low + 1 :]:
            push(src, w_slot(o, m, piece), w_send.at[o, m | b, k], w_recv.at[o, m | b, k], to_t(b))

    def w_across(h, piece):
        k = pieces.index(piece)
        target = origins[h]
        push(
            w_own(target, piece),
            w_slot(c, 0, piece),
            w_send.at[target, 0, k],
            w_recv.at[c, 0, k],
            (d, target * T + t),
        )

    def i_push(o, m, e, part, own, new_m, new_e, peer):
        first, count = part_rows(part)
        src = in_ref.at[pl.ds(first, count)] if own else i_slot(o, m, e, part)
        k = int(part == TAIL_PART)
        push(src, i_slot(o, m, e, part), i_send.at[o, new_m, new_e, k], i_recv.at[o, new_m, new_e, k], peer)

    def i_forward(o, m, e, part, own=False):
        if m & last:
            return
        low = -1
        for b in early:
            if m & b:
                low = early.index(b)
        later = early[low + 1 :]
        if e == 0:
            for b in later:
                i_push(o, m, e, WHOLE, own, m | b, e, to_t(b))
            for shift in range(1, D):
                i_push(o, m, e, HEAD_PART if m else WHOLE, own, m, shift, to_d(shift))
        elif m == 0 or part == TAIL_PART:
            for b in later:
                i_push(o, m, e, TAIL_PART, own, m | b, e, to_t(b))
        i_push(o, m, e, part, own, m | last, e, to_t(last))

    def l_forward(o, src):
        for e in range(1, D):
            push(src, l_slot(o, 0), l_send.at[o, e], l_recv.at[o, e], to_d(e))

    own = [
        pltpu.make_async_copy(
            pack_ref.at[c], w_all.at[pl.ds(pl.multiple_of(seq * depth, depth), depth)], own_sem.at[0]
        ),
        pltpu.make_async_copy(in_ref, i_slot(c, 0, 0, WHOLE), own_sem.at[1]),
        pltpu.make_async_copy(aux_ref, a_slot(0), own_sem.at[3]),
    ]
    for copy in own:
        copy.start()
    height, breadth, frames, channels = start_ref.shape

    def share_rows(l, source):
        push(source.at[height - 1], halos.at[l, 0], h_send.at[l, 0], h_recv.at[l, 0], below)
        push(source.at[0], halos.at[l, 1], h_send.at[l, 1], h_recv.at[l, 1], above)

    share_rows(0, start_ref)
    below_above(in_ref, i_slot(c, 0, 0, WHOLE), zi_send, i_recv.at[c, 0, 0, 0])
    i_forward(c, 0, 0, WHOLE, own=True)
    for shift in range(1, D):
        push(aux_ref, a_slot(0), a_send.at[shift], a_recv.at[shift], to_d(shift))

    def i_event(o, m, e, part=0):
        arrived(i_slot(o, m, e, part), i_recv.at[o, m, e, int(part == TAIL_PART)])
        i_forward(o, m, e, part)

    def iz_event(h):
        o = origins[h]
        slot = i_slot(o, 0, 0, WHOLE)
        arrived(slot, i_recv.at[o, 0, 0, 0])
        peer, guard = along(o)
        push(slot, slot, zi_send.at[1 + h], i_recv.at[o, 0, 0, 0], peer, guard)
        i_forward(o, 0, 0, WHOLE)

    def w_event(h, m, piece):
        o = origins[h]
        slot = w_slot(o, m, piece)
        arrived(slot, w_recv.at[o, m, pieces.index(piece)])
        w_forward(o, m, piece, slot)

    w_pushes = []
    for piece in pieces:
        w_pushes += [(h, piece) for h in range(C - 1, -1, -1)]

    def w_start(count):
        for h, piece in w_pushes[:count]:
            if h:
                w_across(h, piece)
            else:
                w_forward(c, 0, piece, w_own(c, piece))
        del w_pushes[:count]

    def lz_event(h):
        o = origins[h]
        slot = l_slot(o, 0)
        arrived(slot, l_recv.at[o, 0])
        peer, guard = along(o)
        push(slot, slot, zl_send.at[1 + h], l_recv.at[o, 0], peer, guard)
        l_forward(o, slot)

    lanes = 256

    def encode(l, source):
        arrived(halos.at[l, 0], h_recv.at[l, 0])
        arrived(halos.at[l, 1], h_recv.at[l, 1])
        frame_ids = lax.broadcasted_iota(jnp.int32, (frames, lanes), 0)

        def lane_step(j, carry):
            cols = pl.ds(pl.multiple_of(j * lanes, lanes), lanes)
            taps = taps_ref[l, :, cols].astype(jnp.float32)

            def patch(r, w):
                if r < 0:
                    return jnp.where(seq > 0, halos[l, 0, w, :, cols].astype(jnp.float32), 0.0)
                if r == height:
                    return jnp.where(seq < S - 1, halos[l, 1, w, :, cols].astype(jnp.float32), 0.0)
                return source[r, w, :, cols].astype(jnp.float32)

            for r in range(height):
                for w in range(breadth):
                    sums = [None] * 3
                    for b in range(3):
                        for k in range(3):
                            if not 0 <= w + k - 1 < breadth:
                                continue
                            value = patch(r + b - 1, w + k - 1)
                            for a in range(3):
                                tap = 9 * a + 3 * b + k
                                term = value * taps[tap : tap + 1]
                                sums[a] = term if sums[a] is None else sums[a] + term
                    total = sums[2]
                    for a in range(2):
                        moved = pltpu.roll(sums[a], 2 - a, 0)
                        total = total + jnp.where(frame_ids >= 2 - a, moved, 0.0)
                    base = (r * breadth + w) * frames
                    conv[base : base + frames, cols] = total
            return carry

        lax.fori_loop(0, channels // lanes, lane_step, 0)
        summed = conv[...]
        factor = lax.rsqrt(jnp.mean(summed * summed, axis=-1, keepdims=True) + 1e-05)
        gain = gains_ref[l].astype(jnp.float32)
        normed = (summed * factor * gain[None]).astype(jnp.bfloat16)
        projected = jnp.dot(normed, point_ref[l], preferred_element_type=jnp.float32)
        change = gelu(projected)
        for r in range(height):
            for w in range(breadth):
                base = (r * breadth + w) * frames
                value = source[r, w].astype(jnp.float32) + change[base : base + frames]
                value = value.astype(jnp.bfloat16)
                if l + 1 < point_ref.shape[0]:
                    middle[l, r, w] = value
                else:
                    latent_ref[base : base + frames] = value

    def local_events(h):
        o = origins[h]
        for m in near_masks:
            if m:
                i_event(o, m, 0)
        for e in range(1, D):
            i_event(o, 0, e)

    source = start_ref
    for l in range(point_ref.shape[0]):
        with jax.named_scope("encode"):
            encode(l, source)
        if l + 1 < point_ref.shape[0]:
            source = middle.at[l]
            share_rows(l + 1, source)
            w_start(1)
            if l == 0 and C > 1:
                with jax.named_scope("iz1"):
                    iz_event(1)
    below_above(latent_ref, l_slot(c, 0), zl_send, l_recv.at[c, 0])
    l_forward(c, latent_ref)
    latent_copy = pltpu.make_async_copy(latent_ref, l_slot(c, 0), own_sem.at[2])
    latent_copy.start()
    own.append(latent_copy)

    def local_events(h):
        o = origins[h]
        with jax.named_scope("local%d" % h):
            for m in near_masks:
                if m:
                    i_event(o, m, 0)
            for e in range(1, D):
                i_event(o, 0, e)

    def w_events(piece, count):
        with jax.named_scope("w%d_%d" % (pieces.index(piece), count)):
            for m in range(T):
                if (m & ~last).bit_count() + (T if m & last else 0) == count:
                    for h in range(C - 1, -1, -1):
                        if h or m:
                            w_event(h, m, piece)

    w_start(1)
    local_events(0)
    for h in range(1, C):
        if h > 1:
            with jax.named_scope("iz%d" % h):
                iz_event(h)
            w_start(1)
        with jax.named_scope("lz%d" % h):
            lz_event(h)
        local_events(h)
    w_start(len(w_pushes))
    steps = len(early) + 1
    w_todo = []
    for k in range(len(pieces) + steps - 1):
        for count in range(steps):
            if 0 <= k - count < len(pieces):
                w_todo.append((pieces[k - count], count))

    def core_events(e):
        with jax.named_scope("core"):
            for h in range(C):
                for m in near_masks:
                    if m and e:
                        i_event(origins[h], m | last, e, HEAD_PART)
                        i_event(origins[h], m | last, e, TAIL_PART)
                    else:
                        i_event(origins[h], m | last, e)

    def cross_events(e):
        with jax.named_scope("cross"):
            for h in range(C):
                for m in near_masks:
                    if m:
                        i_event(origins[h], m, e, HEAD_PART)
                        i_event(origins[h], m, e, TAIL_PART)

    chunk = math.gcd(in_cols, 512)
    rows = D * tokens

    def embed_block(where, e):
        first = ((d + D - e) % D) * in_cols
        if e == 0:
            squares[where] = jnp.zeros((rows, HEAD), jnp.float32)

        def step(j, carry):
            cols = pl.ds(pl.multiple_of(first + j * chunk, HEAD), chunk)
            z = jnp.dot(lat_all[where], in_all[:, cols], preferred_element_type=jnp.float32)
            z = z + jnp.dot(pick_ref[...], aux_all[:, cols], preferred_element_type=jnp.float32)
            g = gelu(z)
            gain = aux_all[:, cols].astype(jnp.float32)[8:9]
            embeds[where, :, cols] = (g * gain).astype(jnp.bfloat16)
            square = g * g
            part = square[:, :HEAD]
            for k in range(1, chunk // HEAD):
                part = part + square[:, k * HEAD : (k + 1) * HEAD]
            squares[where] += part
            return carry

        with jax.named_scope("embed"):
            lax.fori_loop(0, in_cols // chunk, step, 0)

    if w_todo:
        w_events(*w_todo.pop(0))
    core_events(0)
    for copy in own:
        copy.wait()
    per = -(-(len(w_todo)) // (C * D))
    for e in range(D):
        if e:
            cross_events(e)
            with jax.named_scope("aux"):
                arrived(a_slot(e), a_recv.at[e])
            core_events(e)
        for h in range(C):
            if e == 0:
                with jax.named_scope("lx%d" % h):
                    for k in range(1, D):
                        arrived(l_slot(origins[h], k), l_recv.at[origins[h], k])
            embed_block(origins[h], e)
            for item in w_todo[:per]:
                w_events(*item)
            del w_todo[:per]

    row_ids = lax.broadcasted_iota(jnp.int32, (tokens, tokens), 0)
    col_ids = lax.broadcasted_iota(jnp.int32, (tokens, tokens), 1)
    seen = (row_ids // frames == col_ids // frames) & (row_ids >= col_ids)

    def unit(x):
        return x * lax.rsqrt(jnp.mean(x * x, axis=-1, keepdims=True) + 1e-06)

    def mix_block(where, g):
        first, count = w_cols[g]
        total = jnp.dot(
            embeds[where], w_all[:, first : first + count], preferred_element_type=jnp.float32
        )
        mean = jnp.sum(squares[where], axis=-1, keepdims=True) / DIM
        total = total * lax.rsqrt(mean + 1e-05)
        if g == 0:
            keys[where] = unit(total[:, :HEAD]).astype(jnp.bfloat16)
            values[where] = total[:, HEAD : 2 * HEAD].astype(jnp.bfloat16)
        key, value = keys[where], values[where]
        for at in range(2 * HEAD if g == 0 else 0, count, HEAD):
            query = (unit(total[:, at : at + HEAD]) * HEAD**-0.5).astype(jnp.bfloat16)
            to = first + at - 2 * HEAD
            for clip in range(D):
                span = slice(clip * tokens, (clip + 1) * tokens)
                score = lax.dot_general(
                    query[span],
                    key[span],
                    (((1,), (1,)), ((), ())),
                    preferred_element_type=jnp.float32,
                )
                raised = jnp.where(seen, jnp.exp(score), 0.0)
                shares = raised / jnp.sum(raised, axis=-1, keepdims=True)
                result = jnp.dot(
                    shares.astype(jnp.bfloat16), value[span], preferred_element_type=jnp.float32
                )
                mixed[where, span, to : to + HEAD] = result.astype(jnp.bfloat16)

    def out_cols(g):
        first, count = w_cols[g]
        return (0, count - 2 * HEAD) if g == 0 else (first - 2 * HEAD, count)

    def send_of(where, g):
        first, count = out_cols(g)
        return pltpu.make_async_remote_copy(
            src_ref=mixed.at[where, :, pl.ds(first, count)],
            dst_ref=out_ref.at[:, pl.ds(pl.multiple_of(c * qcols + first, HEAD), count)],
            send_sem=o_send.at[where, g],
            recv_sem=o_recv.at[c, g],
            device_id=(d, where * T + t),
            device_id_type=MESH,
        )

    for g in range(2):
        for piece in pieces:
            if piece[0] == g:
                for count in range(T, T + steps):
                    w_events(piece, count)
        for h in range(C - 1, 0, -1):
            with jax.named_scope("mix"):
                mix_block(origins[h], g)
            send_of(origins[h], g).start()
    for g in range(2):
        with jax.named_scope("mix"):
            mix_block(c, g)
    keep = pltpu.make_async_copy(
        mixed.at[c], out_ref.at[:, pl.ds(pl.multiple_of(c * qcols, HEAD), qcols)], own_sem.at[0]
    )
    keep.start()
    with jax.named_scope("tail"):
        for g in range(2):
            first, count = out_cols(g)
            for h in range(C - 1, 0, -1):
                send_of(origins[h], g).wait_send()
                column = origins[h] * qcols + first
                arrived(
                    out_ref.at[:, pl.ds(pl.multiple_of(column, HEAD), count)], o_recv.at[origins[h], g]
                )
        keep.wait()
    for copy, guard in sends:
        if guard is None:
            copy.wait_send()
        else:
            pl.when(guard)(copy.wait_send)


def body(
    tiles,
    patch_index,
    pos_table,
    depth_kernel,
    enc_gain,
    point_weight,
    action_ids,
    w_in,
    action_table,
    dyn_gain,
    w_query,
    w_keyval,
    seq_order,
):
    clip_local, frames, height, breadth, channels = tiles.shape
    positions = pos_table.shape[0]
    blocks = depth_kernel.shape[0]
    D, S = lax.axis_size("dp"), lax.axis_size("seq")
    kv_local = w_keyval.shape[2] // HEAD
    C = math.gcd(kv_local, S)
    T = S // C
    assert T & (T - 1) == 0 and T > 1 and clip_local == 1 and kv_local == C
    group = Q_HEADS // KV_HEADS
    depth = w_query.shape[0]
    frames_first = (0, 3, 1, 2, 4)

    flat_index = patch_index.reshape(-1)
    position_pick = (flat_index[:, None] == jnp.arange(positions, dtype=jnp.int32)[None, :]).astype(
        jnp.bfloat16
    )
    placed = jnp.dot(position_pick, pos_table, preferred_element_type=jnp.float32).reshape(
        tiles.shape
    )
    hidden = (tiles.astype(jnp.float32) + placed).astype(jnp.bfloat16)
    start = hidden[0].transpose(1, 2, 0, 3)

    cells = height * breadth
    tokens = frames * cells
    pack = jnp.concatenate(
        [
            w_keyval.reshape(depth, 2, C, -1).transpose(2, 0, 1, 3).reshape(C, depth, -1),
            w_query.reshape(depth, C, -1).transpose(1, 0, 2),
        ],
        axis=2,
    )
    actions = action_table.shape[0]
    assert actions == 8
    aux = jnp.concatenate(
        [action_table, dyn_gain[None], jnp.zeros((7, action_table.shape[1]), jnp.bfloat16)], axis=0
    )
    pick = (
        jnp.tile(action_ids[:, None, :], (1, cells, 1)).reshape(-1)[:, None] == jnp.arange(16, dtype=jnp.int32)[None]
    ).astype(jnp.bfloat16)
    width = pack.shape[2]
    qcols = group * HEAD
    bf16, f32 = jnp.bfloat16, jnp.float32
    dma = pltpu.SemaphoreType.DMA
    out = pl.pallas_call(
        functools.partial(window_kernel, (D, C, T, (2 + group // 2) * HEAD)),
        out_shape=jax.ShapeDtypeStruct((D * tokens, C * qcols), bf16),
        in_specs=[pl.BlockSpec(memory_space=pltpu.VMEM)] * 8,
        out_specs=pl.BlockSpec(memory_space=pltpu.VMEM),
        scratch_shapes=[
            pltpu.VMEM((S * depth, width), bf16),
            pltpu.VMEM((channels, DIM), bf16),
            pltpu.VMEM((16, DIM), bf16),
            pltpu.VMEM((C, D * tokens, channels), bf16),
            pltpu.VMEM((C, D * tokens, DIM), bf16),
            pltpu.VMEM((C, D * tokens, HEAD), f32),
            pltpu.VMEM((C, D * tokens, qcols), bf16),
            pltpu.VMEM((C, D * tokens, HEAD), bf16),
            pltpu.VMEM((C, D * tokens, HEAD), bf16),
            pltpu.VMEM((blocks, 2, breadth, frames, channels), bf16),
            pltpu.VMEM((max(blocks - 1, 1), height, breadth, frames, channels), bf16),
            pltpu.VMEM((tokens, channels), f32),
            pltpu.VMEM((tokens, channels), bf16),
            dma((blocks, 2)),
            dma((blocks, 2)),
            dma((C, T, 4)),
            dma((C, T, 4)),
            dma((C, T, D, 2)),
            dma((C, T, D, 2)),
            dma((C, D)),
            dma((C, D)),
            dma((D,)),
            dma((D,)),
            dma((C, 2)),
            dma((C, 2)),
            dma((4,)),
            dma((C + 1,)),
            dma((C + 1,)),
        ],
        compiler_params=pltpu.CompilerParams(
            collective_id=0, has_side_effects=True, vmem_limit_bytes=60 * 1024 * 1024
        ),
    )(pack, w_in, aux, start, depth_kernel, enc_gain, point_weight, pick)
    out = out.reshape(D, height, breadth, frames, -1).transpose(frames_first)
    return jnp.take(out, seq_order, axis=3)


def solution(mesh):
    placed = (
        P("dp", None, "seq", None, None),
        P("dp", None, "seq", None),
        P(),
        P(),
        P(),
        P(),
        P(),
        P("seq", "dp"),
        P(None, "dp"),
        P("dp"),
        P("seq", "dp"),
        P("seq", None, "dp"),
        P(),
    )
    return jax.shard_map(
        body,
        mesh=mesh,
        in_specs=placed,
        out_specs=P(None, None, "seq", None, "dp"),
        check_vma=False,
    )
```

```python
import functools
import math

import jax
import jax.numpy as jnp
from jax import lax
from jax.experimental import pallas as pl
from jax.experimental.pallas import tpu as pltpu
from jax.sharding import PartitionSpec as P

DIM = 5120
HEAD = 128
Q_HEADS = 40
KV_HEADS = 8
MESH = pl.DeviceIdType.MESH


def gelu(z):
    half = 0.5 * z
    return half + half * jnp.tanh(z * (0.7978845608028654 + 0.035677408136300125 * (z * z)))


def flipped(t, mask, bits):
    for bit in bits:
        if mask & bit:
            t = t + bit - 2 * bit * ((t // bit) % 2)
    return t


def window_kernel(
    sizes,
    query_ref,
    keyval_ref,
    in_ref,
    action_ref,
    scale_ref,
    tiles_ref,
    place_ref,
    table_ref,
    taps_ref,
    gains_ref,
    point_hbm,
    ids_ref,
    order_ref,
    out_ref,
    w_all,
    in_all,
    aux_all,
    lat_all,
    embeds,
    squares,
    mixed,
    keys,
    values,
    halos,
    middle,
    conv,
    latent_ref,
    rough,
    start_ref,
    point_ref,
    aux_ref,
    kv_pack,
    place_row,
    ids_row,
    h_send,
    h_recv,
    w_send,
    w_recv,
    i_send,
    i_recv,
    l_send,
    l_recv,
    a_send,
    a_recv,
    o_send,
    o_recv,
    own_sem,
    zi_send,
    zl_send,
):
    D, C, T, edges = sizes
    d = lax.axis_index("dp")
    seq = lax.axis_index("seq")
    c = seq // T
    t = seq % T
    bits = []
    bit = T // 2
    while bit:
        bits.append(bit)
        bit //= 2
    early, last = bits[:-1], bits[-1]
    near_masks = [m for m in range(T) if not m & last]
    near_masks.sort(key=lambda m: m.bit_count())
    depth = query_ref.shape[0]
    in_rows, in_cols = in_ref.shape
    tokens = latent_ref.shape[0]
    rows = D * tokens
    banks = min(C, 2)
    bank = C // banks
    bank_rows = bank * rows
    far = (banks - 1) - c // bank
    near = c // bank
    group = Q_HEADS // KV_HEADS
    qcols = group * HEAD

    orders = [
        sorted(range(C), key=lambda o, i=i: (abs(o - i), o if 2 * i < C else -o)) for i in range(C)
    ]

    def nearest(h):
        value = orders[0][h]
        for i in range(1, C):
            value = jnp.where(c == i, orders[i][h], value)
        return value

    origins = [c] + [nearest(h) for h in range(1, C)]

    def to_c(shift):
        return (d, ((c + shift) % C) * T + t)

    def to_t(bit):
        return (d, c * T + flipped(t, bit, bits))

    def to_d(shift):
        return ((d + shift) % D, seq)

    peers = [to_c(s) for s in range(1, C)] + [to_t(b) for b in bits] + [to_d(s) for s in range(1, D)]
    S = C * T
    above, below = (d, (seq + S - 1) % S), (d, (seq + 1) % S)
    peers += [above, below]
    own = [
        pltpu.make_async_copy(point_hbm, point_ref, own_sem.at[4]),
        pltpu.make_async_copy(
            in_ref,
            in_all.at[
                pl.ds(pl.multiple_of(seq * in_rows, in_rows), in_rows),
                pl.ds(pl.multiple_of(d * in_cols, HEAD), in_cols),
            ],
            own_sem.at[1],
        ),
        pltpu.make_async_copy(
            query_ref.at[:, pl.ds(pl.multiple_of(c * qcols, HEAD), qcols)],
            w_all.at[pl.ds(pl.multiple_of(seq * depth, depth), depth), pl.ds(2 * HEAD, qcols)],
            own_sem.at[0],
        ),
    ]
    point_copy = own.pop(0)
    point_copy.start()
    for copy in own:
        copy.start()
    height, breadth, frames, channels = start_ref.shape
    with jax.named_scope("place"):
        positions = table_ref.shape[0]
        for r in range(height):
            for w in range(breadth):
                base = (r * breadth + w) * frames
                place_row[:, base : base + frames] = place_ref[0, r, w : w + 1, :]
        for k in range(D):
            ids_row[:, k * frames : (k + 1) * frames] = ids_ref[k : k + 1, :]
        chosen = place_row[...] == lax.broadcasted_iota(jnp.int32, (positions, tokens), 0)
        placed = lax.dot_general(
            jnp.where(chosen, 1.0, 0.0).astype(jnp.bfloat16),
            table_ref[...],
            (((0,), (0,)), ((), ())),
            preferred_element_type=jnp.float32,
        )
        for r in range(height):
            for w in range(breadth):
                base = (r * breadth + w) * frames
                tile = tiles_ref[0, :, r, w, :].astype(jnp.float32)
                start_ref[r, w] = (tile + placed[base : base + frames]).astype(jnp.bfloat16)
        actions = action_ref.shape[0]
        aux_ref[:actions] = action_ref[...]
        for k in range(in_cols // HEAD):
            aux_ref[actions:, k * HEAD : (k + 1) * HEAD] = jnp.broadcast_to(
                scale_ref[k : k + 1, :], (16 - actions, HEAD)
            )

    with jax.named_scope("barrier"):
        barrier = pltpu.get_barrier_semaphore()
        for peer in peers:
            pl.semaphore_signal(barrier, inc=1, device_id=peer, device_id_type=MESH)
        pl.semaphore_wait(barrier, len(peers))

    log = []
    waiting = []

    def run(guard, event, *args):
        if not waiting:
            log.append((guard, event, args))
        if guard is None:
            event(*args)
        else:
            pl.when(guard)(functools.partial(event, *args))

    def push(src, dst, send_sem, recv_sem, peer):
        copy = pltpu.make_async_remote_copy(
            src_ref=src,
            dst_ref=dst,
            send_sem=send_sem,
            recv_sem=recv_sem,
            device_id=peer,
            device_id_type=MESH,
        )
        if waiting:
            copy.wait_send()
        else:
            copy.start()

    def arrived(ref, sem):
        if not waiting:
            pltpu.make_async_copy(ref, ref, sem).wait()

    w_cols = [(first, last_col - first) for first, last_col in zip(edges, edges[1:])]
    stages = len(w_cols)
    pieces = [(0, 0, 2 * HEAD)]
    pieces += [(g, max(first, 2 * HEAD), min(count, first + count - 2 * HEAD)) for g, (first, count) in enumerate(w_cols)]

    def w_slot(o, m, piece):
        g, first, count = piece
        origin = o * T + flipped(t, m, bits)
        return w_all.at[
            pl.ds(pl.multiple_of(origin * depth, depth), depth), pl.ds(first, count)
        ]

    def w_own(target, piece):
        g, first, count = piece
        if first == 0:
            return kv_pack.at[target]
        column = target * qcols + first - 2 * HEAD
        return query_ref.at[:, pl.ds(pl.multiple_of(column, HEAD), count)]

    split = in_rows // 2
    WHOLE, HEAD_PART, TAIL_PART = 0, 1, 2

    def part_rows(part):
        return ((0, in_rows), (0, split), (split, in_rows - split))[part]

    def i_slot(o, m, e, part):
        first, count = part_rows(part)
        origin = o * T + flipped(t, m, bits)
        column = ((d + D - e) % D) * in_cols
        return in_all.at[
            pl.ds(pl.multiple_of(origin * in_rows + first, math.gcd(in_rows, split)), count),
            pl.ds(pl.multiple_of(column, HEAD), in_cols),
        ]

    def l_slot(o, e):
        row = ((d + D - e) % D) * tokens
        return lat_all.at[pl.ds(pl.multiple_of(o * rows + row, tokens), tokens)]

    def a_slot(e):
        column = ((d + D - e) % D) * in_cols
        return aux_all.at[:, pl.ds(pl.multiple_of(column, HEAD), in_cols)]

    hops = [(k, way) for k in range(1, C) for way in (1, -1)]

    def hop_origin(k, way):
        return c - way * k

    def hop_guard(k, way):
        return c >= k if way > 0 else c + k < C

    def onward(way):
        return (d, (c + way) * T + t), (c + 1 < C if way > 0 else c >= 1)

    def z_own(src, dst, send_sems, recv_sem):
        for k, way in enumerate((1, -1)):
            if C > 1:
                peer, guard = onward(way)
                pl.when(guard)(functools.partial(push, src, dst, send_sems.at[k], recv_sem, peer))

    def z_hop(slot, send_sem, recv_sem, way):
        peer, guard = onward(way)
        pl.when(guard)(functools.partial(push, slot, slot, send_sem, recv_sem, peer))

    def w_forward(o, m, piece, src):
        k = pieces.index(piece)
        low = -1
        for b in bits:
            if m & b:
                low = bits.index(b)
        for b in bits[low + 1 :]:
            push(src, w_slot(o, m, piece), w_send.at[o, m | b, k], w_recv.at[o, m | b, k], to_t(b))

    def w_across(h, piece):
        k = pieces.index(piece)
        target = origins[h]
        push(
            w_own(target, piece),
            w_slot(c, 0, piece),
            w_send.at[target, 0, k],
            w_recv.at[c, 0, k],
            (d, target * T + t),
        )

    def i_push(o, m, e, part, own, new_m, new_e, peer):
        first, count = part_rows(part)
        src = in_ref.at[pl.ds(first, count)] if own else i_slot(o, m, e, part)
        k = int(part == TAIL_PART)
        push(src, i_slot(o, m, e, part), i_send.at[o, new_m, new_e, k], i_recv.at[o, new_m, new_e, k], peer)

    def i_forward(o, m, e, part, own=False):
        if m & last:
            return
        low = -1
        for b in early:
            if m & b:
                low = early.index(b)
        later = early[low + 1 :]
        if e == 0:
            for b in later:
                i_push(o, m, e, WHOLE, own, m | b, e, to_t(b))
            for shift in range(1, D):
                i_push(o, m, e, HEAD_PART if m else WHOLE, own, m, shift, to_d(shift))
        elif m == 0 or part == TAIL_PART:
            for b in later:
                i_push(o, m, e, TAIL_PART, own, m | b, e, to_t(b))
        i_push(o, m, e, part, own, m | last, e, to_t(last))

    def l_forward(o, src):
        for e in range(1, D):
            push(src, l_slot(o, 0), l_send.at[o, e], l_recv.at[o, e], to_d(e))

    def share_rows(l, source):
        push(source.at[height - 1], halos.at[l, 0], h_send.at[l, 0], h_recv.at[l, 0], below)
        push(source.at[0], halos.at[l, 1], h_send.at[l, 1], h_recv.at[l, 1], above)

    def start_own():
        z_own(in_ref, i_slot(c, 0, 0, WHOLE), zi_send, i_recv.at[c, 0, 0, 0])
        i_forward(c, 0, 0, WHOLE, True)
        for shift in range(1, D):
            push(aux_ref, a_slot(0), a_send.at[shift], a_recv.at[shift], to_d(shift))

    own.append(pltpu.make_async_copy(aux_ref, a_slot(0), own_sem.at[3]))
    own[-1].start()
    run(None, share_rows, 0, start_ref)
    run(None, start_own)

    def i_event(o, m, e, part=0):
        arrived(i_slot(o, m, e, part), i_recv.at[o, m, e, int(part == TAIL_PART)])
        i_forward(o, m, e, part)

    def iz_event(k, way):
        o = hop_origin(k, way)
        slot = i_slot(o, 0, 0, WHOLE)
        arrived(slot, i_recv.at[o, 0, 0, 0])
        z_hop(slot, zi_send.at[2 * k + (way > 0)], i_recv.at[o, 0, 0, 0], way)
        i_forward(o, 0, 0, WHOLE)

    def lz_event(k, way):
        o = hop_origin(k, way)
        slot = l_slot(o, 0)
        arrived(slot, l_recv.at[o, 0])
        z_hop(slot, zl_send.at[2 * k + (way > 0)], l_recv.at[o, 0], way)
        l_forward(o, slot)

    def local_event(k, way):
        o = hop_origin(k, way)
        for m in near_masks:
            if m:
                i_event(o, m, 0)
        for e in range(1, D):
            i_event(o, 0, e)

    def both_ways(event, k):
        with jax.named_scope("%s%d" % (event.__name__[:2], k)):
            for way in (1, -1) if 0 < k < C else ():
                run(hop_guard(k, way), event, k, way)

    def w_event(h, m, piece):
        o = origins[h]
        slot = w_slot(o, m, piece)
        arrived(slot, w_recv.at[o, m, pieces.index(piece)])
        w_forward(o, m, piece, slot)

    def w_forward_own(piece):
        w_forward(c, 0, piece, w_own(c, piece))

    w_pushes = []
    for piece in pieces:
        w_pushes += [(h, piece) for h in range(C - 1, -1, -1)]

    def w_start(count):
        for h, piece in w_pushes[:count]:
            if h:
                run(None, w_across, h, piece)
            else:
                run(None, w_forward_own, piece)
        del w_pushes[:count]

    lanes = 256

    def encode(l, source):
        arrived(halos.at[l, 0], h_recv.at[l, 0])
        arrived(halos.at[l, 1], h_recv.at[l, 1])
        frame_ids = lax.broadcasted_iota(jnp.int32, (frames, lanes), 0)

        def lane_step(j, carry):
            cols = pl.ds(pl.multiple_of(j * lanes, lanes), lanes)
            taps = [taps_ref[k, l : l + 1, cols].astype(jnp.float32) for k in range(27)]

            def patch(r, w):
                if r < 0:
                    return jnp.where(seq > 0, halos[l, 0, w, :, cols].astype(jnp.float32), 0.0)
                if r == height:
                    return jnp.where(seq < S - 1, halos[l, 1, w, :, cols].astype(jnp.float32), 0.0)
                return source[r, w, :, cols].astype(jnp.float32)

            for r in range(height):
                for w in range(breadth):
                    sums = [None] * 3
                    for b in range(3):
                        for k in range(3):
                            if not 0 <= w + k - 1 < breadth:
                                continue
                            value = patch(r + b - 1, w + k - 1)
                            for a in range(3):
                                tap = 9 * a + 3 * b + k
                                term = value * taps[tap]
                                sums[a] = term if sums[a] is None else sums[a] + term
                    total = sums[2]
                    for a in range(2):
                        moved = pltpu.roll(sums[a], 2 - a, 0)
                        total = total + jnp.where(frame_ids >= 2 - a, moved, 0.0)
                    base = (r * breadth + w) * frames
                    conv[base : base + frames, cols] = total
            return carry

        lax.fori_loop(0, channels // lanes, lane_step, 0)
        summed = conv[...]
        factor = lax.rsqrt(jnp.mean(summed * summed, axis=-1, keepdims=True) + 1e-05)
        gain = gains_ref[l].astype(jnp.float32)
        normed = (summed * factor * gain[None]).astype(jnp.bfloat16)
        projected = jnp.dot(normed, point_ref[l], preferred_element_type=jnp.float32)
        change = gelu(projected)
        for r in range(height):
            for w in range(breadth):
                base = (r * breadth + w) * frames
                value = source[r, w].astype(jnp.float32) + change[base : base + frames]
                value = value.astype(jnp.bfloat16)
                if l + 1 < point_ref.shape[0]:
                    middle[l, r, w] = value
                else:
                    rough[base : base + frames] = value

    def local_events(h):
        o = origins[h]
        for m in near_masks:
            if m:
                i_event(o, m, 0)
        for e in range(1, D):
            i_event(o, 0, e)

    point_copy.wait()
    source = start_ref
    for l in range(point_ref.shape[0]):
        with jax.named_scope("encode"):
            encode(l, source)
        if l + 1 < point_ref.shape[0]:
            source = middle.at[l]
            run(None, share_rows, l + 1, source)
        if l == 0:
            both_ways(iz_event, 1)
            run(None, local_event, 0, 1)

    with jax.named_scope("order"):
        row_ids = lax.broadcasted_iota(jnp.int32, (tokens, tokens), 0)
        col_ids = lax.broadcasted_iota(jnp.int32, (tokens, tokens), 1)
        row_cells, col_cells = row_ids // frames, col_ids // frames
        wanted = row_cells // breadth * breadth
        for w in range(breadth):
            wanted = wanted + jnp.where(row_cells % breadth == w, order_ref[w], 0)
        moved = (wanted == col_cells) & (row_ids % frames == col_ids % frames)
        latent_ref[...] = jnp.dot(
            jnp.where(moved, 1.0, 0.0).astype(jnp.bfloat16), rough[...], preferred_element_type=jnp.float32
        ).astype(jnp.bfloat16)

    def start_latent():
        z_own(latent_ref, l_slot(c, 0), zl_send, l_recv.at[c, 0])
        l_forward(c, latent_ref)

    run(None, start_latent)
    latent_copy = pltpu.make_async_copy(latent_ref, l_slot(c, 0), own_sem.at[2])
    latent_copy.start()
    own.append(latent_copy)

    def w_events(piece, count):
        with jax.named_scope("w%d_%d" % (pieces.index(piece), count)):
            for m in range(T):
                if (m & ~last).bit_count() + (T if m & last else 0) == count:
                    for h in range(C - 1, -1, -1):
                        if h or m:
                            run(None, w_event, h, m, piece)

    both_ways(iz_event, 2)
    with jax.named_scope("kv"):
        for o in range(C):
            for k in range(2):
                kv_pack[o, :, k * HEAD : (k + 1) * HEAD] = keyval_ref[:, k, o * HEAD : (o + 1) * HEAD]
        own.append(pltpu.make_async_copy(kv_pack.at[c], w_slot(c, 0, pieces[0]), own_sem.at[5]))
        own[-1].start()
    both_ways(local_event, 1)
    both_ways(lz_event, 1)
    both_ways(iz_event, 3)
    both_ways(lz_event, 2)
    w_start(2)
    both_ways(local_event, 2)
    w_start(2)
    both_ways(lz_event, 3)
    w_start(4)
    both_ways(local_event, 3)
    for k in range(4, C):
        for event in (iz_event, local_event, lz_event):
            both_ways(event, k)
    w_start(len(w_pushes))
    steps = len(early) + 1
    w_todo = [(k + 2.5 * count, k, count) for k in range(len(pieces)) for count in range(steps)]
    w_todo = [(pieces[k], count) for _, k, count in sorted(w_todo)]

    def core_events(e):
        with jax.named_scope("core"):
            for h in range(C):
                for m in near_masks:
                    if m and e:
                        run(None, i_event, origins[h], m | last, e, HEAD_PART)
                        run(None, i_event, origins[h], m | last, e, TAIL_PART)
                    else:
                        run(None, i_event, origins[h], m | last, e)

    def cross_events(e):
        with jax.named_scope("cross"):
            for h in range(C):
                for m in near_masks:
                    if m:
                        run(None, i_event, origins[h], m, e, HEAD_PART)
                        run(None, i_event, origins[h], m, e, TAIL_PART)

    chunk = in_cols // 2 if in_cols % (2 * HEAD) == 0 else in_cols
    chosen = ids_row[...] == lax.broadcasted_iota(jnp.int32, (16, D * frames), 0)
    picked = jnp.where(chosen, 1.0, 0.0).astype(jnp.bfloat16)

    def rows_of(which):
        return pl.ds(pl.multiple_of(which * bank_rows, bank_rows), bank_rows)

    def embed_bank(which, e):
        at = rows_of(which)
        first = ((d + D - e) % D) * in_cols
        if e == 0:
            squares[at] = jnp.zeros((bank_rows, HEAD), jnp.float32)

        def step(j, carry):
            cols = pl.ds(pl.multiple_of(first + j * chunk, HEAD), chunk)
            z = jnp.dot(lat_all[at], in_all[:, cols], preferred_element_type=jnp.float32)
            action = lax.dot_general(
                picked,
                aux_all[:, cols],
                (((0,), (0,)), ((), ())),
                preferred_element_type=jnp.float32,
            )
            action = jnp.broadcast_to(
                action.reshape(1, D, 1, frames, chunk),
                (bank, D, tokens // frames, frames, chunk),
            )
            g = gelu(z + action.reshape(bank_rows, chunk))
            gain = aux_all[:, cols].astype(jnp.float32)[8:9]
            embeds[at, cols] = (g * gain).astype(jnp.bfloat16)
            square = g * g
            part = square[:, :HEAD]
            for k in range(1, chunk // HEAD):
                part = part + square[:, k * HEAD : (k + 1) * HEAD]
            squares[at] += part
            return carry

        with jax.named_scope("embed"):
            lax.fori_loop(0, in_cols // chunk, step, 0)

    def take_w(count):
        for item in w_todo[:count]:
            w_events(*item)
        del w_todo[:count]

    core_events(0)
    take_w(1)
    for copy in own:
        copy.wait()
    with jax.named_scope("lx"):
        for h in range(C):
            for k in range(1, D):
                arrived(l_slot(origins[h], k), l_recv.at[origins[h], k])
    embed_bank(far, 0)
    take_w(1)
    if banks > 1:
        embed_bank(near, 0)
    for e in range(1, D):
        cross_events(e)
        take_w(2)
        with jax.named_scope("aux"):
            arrived(a_slot(e), a_recv.at[e])
        core_events(e)
        embed_bank(far, e)
        take_w(2)
        if banks > 1:
            embed_bank(near, e)

    def need_w(g):
        with jax.named_scope("need"):
            while any(piece[0] <= g for piece, count in w_todo):
                take_w(1)
            for piece in pieces:
                if piece[0] == g:
                    for count in range(T, T + steps):
                        w_events(piece, count)

    seen = (row_ids // frames == col_ids // frames) & (row_ids >= col_ids)

    pair = jnp.where(
        lax.broadcasted_iota(jnp.int32, (2 * HEAD, 2 * HEAD), 0) // HEAD
        == lax.broadcasted_iota(jnp.int32, (2 * HEAD, 2 * HEAD), 1) // HEAD,
        1.0,
        0.0,
    ).astype(jnp.bfloat16)

    def unit(x):
        width = x.shape[1]
        total = jnp.dot(
            (x * x).astype(jnp.bfloat16), pair[:width, :width], preferred_element_type=jnp.float32
        )
        return x * lax.rsqrt(total * (1.0 / HEAD) + 1e-06)

    def mix_bank(which, g):
        first, count = w_cols[g]
        base = which * bank_rows
        at = rows_of(which)
        total = jnp.dot(
            embeds[at], w_all[:, first : first + count], preferred_element_type=jnp.float32
        )
        mean = jnp.sum(squares[at], axis=-1, keepdims=True) / DIM
        total = total * lax.rsqrt(mean + 1e-05)
        if g == 0:
            keys[at] = unit(total[:, :HEAD]).astype(jnp.bfloat16)
            values[at, :HEAD] = total[:, HEAD : 2 * HEAD].astype(jnp.bfloat16)
            values[at, HEAD:] = jnp.ones((bank_rows, HEAD), jnp.bfloat16)
        key, value = keys[at], values[at]
        left = 2 * HEAD if g == 0 else 0
        while left < count:
            width = min(2 * HEAD, count - left)
            query = (unit(total[:, left : left + width]) * HEAD**-0.5).astype(jnp.bfloat16)
            for inner in range(0, width, HEAD):
                to = first + left + inner - 2 * HEAD
                spans = [slice(i, i + tokens) for i in range(0, bank_rows, tokens)]
                scores = [
                    lax.dot_general(
                        query[span, inner : inner + HEAD],
                        key[span],
                        (((1,), (1,)), ((), ())),
                        preferred_element_type=jnp.float32,
                    )
                    for span in spans
                ]
                raised = [
                    jnp.where(seen, jnp.exp(score), 0.0).astype(jnp.bfloat16) for score in scores
                ]
                for i, span in enumerate(spans):
                    both = jnp.dot(raised[i], value[span], preferred_element_type=jnp.float32)
                    result = (both[:, :HEAD] / both[:, HEAD:]).astype(jnp.bfloat16)
                    mixed[pl.ds(pl.multiple_of(base + i * tokens, tokens), tokens), to : to + HEAD] = result
            left += width

    def out_cols(g):
        first, count = w_cols[g]
        return (0, count - 2 * HEAD) if g == 0 else (first - 2 * HEAD, count)

    def block_rows(where):
        return pl.ds(pl.multiple_of(where * rows, rows), rows)

    def send_of(where, g):
        first, count = out_cols(g)
        return pltpu.make_async_remote_copy(
            src_ref=mixed.at[block_rows(where), pl.ds(first, count)],
            dst_ref=out_ref.at[:, pl.ds(pl.multiple_of(c * qcols + first, HEAD), count)],
            send_sem=o_send.at[where, g],
            recv_sem=o_recv.at[c, g],
            device_id=(d, where * T + t),
            device_id_type=MESH,
        )

    far_blocks = [far * bank + j for j in range(bank)] if banks > 1 else []
    near_blocks = [near * bank + (c + j) % bank for j in range(1, bank)]

    for g in range(stages):
        need_w(g)
        for which, blocks in ((far, far_blocks), (near, near_blocks))[2 - banks :]:
            with jax.named_scope("mix"):
                mix_bank(which, g)
            for where in blocks:
                send_of(where, g).start()
    keep = pltpu.make_async_copy(
        mixed.at[block_rows(c)],
        out_ref.at[:, pl.ds(pl.multiple_of(c * qcols, HEAD), qcols)],
        own_sem.at[0],
    )
    keep.start()
    with jax.named_scope("tail"):
        for g in range(stages):
            first, count = out_cols(g)
            for where in near_blocks + far_blocks:
                send_of(where, g).wait_send()
                column = where * qcols + first
                arrived(
                    out_ref.at[:, pl.ds(pl.multiple_of(column, HEAD), count)], o_recv.at[where, g]
                )
        keep.wait()
    waiting.append(True)
    for guard, event, args in log:
        run(guard, event, *args)


def body(
    tiles,
    patch_index,
    pos_table,
    depth_kernel,
    enc_gain,
    point_weight,
    action_ids,
    w_in,
    action_table,
    dyn_gain,
    w_query,
    w_keyval,
    seq_order,
):
    clip_local, frames, height, breadth, channels = tiles.shape
    positions = pos_table.shape[0]
    blocks = depth_kernel.shape[0]
    D, S = lax.axis_size("dp"), lax.axis_size("seq")
    kv_local = w_keyval.shape[2] // HEAD
    C = math.gcd(kv_local, S)
    T = S // C
    assert T & (T - 1) == 0 and T > 1 and clip_local == 1 and kv_local == C
    group = Q_HEADS // KV_HEADS
    depth = w_query.shape[0]

    cells = height * breadth
    tokens = frames * cells
    assert action_table.shape[0] == 8 and depth_kernel.shape[1] == 27
    width = (2 + group) * HEAD
    qcols = group * HEAD
    bf16, f32 = jnp.bfloat16, jnp.float32
    dma = pltpu.SemaphoreType.DMA
    out = pl.pallas_call(
        functools.partial(window_kernel, (D, C, T, [x * HEAD for x in (0, 2 + group // 2, 1 + group, 2 + group)])),
        out_shape=jax.ShapeDtypeStruct((D * tokens, C * qcols), bf16),
        in_specs=[
            pl.BlockSpec(memory_space=space)
            for space in [pl.ANY, pltpu.VMEM, pl.ANY]
            + [pltpu.VMEM] * 7
            + [pl.ANY, pltpu.VMEM, pltpu.SMEM]
        ],
        out_specs=pl.BlockSpec(memory_space=pltpu.VMEM),
        scratch_shapes=[
            pltpu.VMEM((S * depth, width), bf16),
            pltpu.VMEM((channels, DIM), bf16),
            pltpu.VMEM((16, DIM), bf16),
            pltpu.VMEM((C * D * tokens, channels), bf16),
            pltpu.VMEM((C * D * tokens, DIM), bf16),
            pltpu.VMEM((C * D * tokens, HEAD), f32),
            pltpu.VMEM((C * D * tokens, qcols), bf16),
            pltpu.VMEM((C * D * tokens, HEAD), bf16),
            pltpu.VMEM((C * D * tokens, 2 * HEAD), bf16),
            pltpu.VMEM((blocks, 2, breadth, frames, channels), bf16),
            pltpu.VMEM((max(blocks - 1, 1), height, breadth, frames, channels), bf16),
            pltpu.VMEM((tokens, channels), f32),
            pltpu.VMEM((tokens, channels), bf16),
            pltpu.VMEM((tokens, channels), bf16),
            pltpu.VMEM((height, breadth, frames, channels), bf16),
            pltpu.VMEM(point_weight.shape, bf16),
            pltpu.VMEM((16, w_in.shape[1]), bf16),
            pltpu.VMEM((C, depth, 2 * HEAD), bf16),
            pltpu.VMEM((1, tokens), jnp.int32),
            pltpu.VMEM((1, D * frames), jnp.int32),
            dma((blocks, 2)),
            dma((blocks, 2)),
            dma((C, T, 4)),
            dma((C, T, 4)),
            dma((C, T, D, 2)),
            dma((C, T, D, 2)),
            dma((C, D)),
            dma((C, D)),
            dma((D,)),
            dma((D,)),
            dma((C, 3)),
            dma((C, 3)),
            dma((6,)),
            dma((2 * C,)),
            dma((2 * C,)),
        ],
        compiler_params=pltpu.CompilerParams(
            collective_id=0, has_side_effects=True, vmem_limit_bytes=60 * 1024 * 1024
        ),
    )(
        w_query,
        w_keyval,
        w_in,
        action_table,
        dyn_gain.reshape(-1, HEAD),
        tiles,
        patch_index.transpose(0, 2, 3, 1),
        pos_table,
        depth_kernel.transpose(1, 0, 2),
        enc_gain,
        point_weight,
        action_ids,
        seq_order,
    )
    return out.reshape(D, height, breadth, frames, -1).transpose(0, 3, 1, 2, 4)


def solution(mesh):
    placed = (
        P("dp", None, "seq", None, None),
        P("dp", None, "seq", None),
        P(),
        P(),
        P(),
        P(),
        P(),
        P("seq", "dp"),
        P(None, "dp"),
        P("dp"),
        P("seq", "dp"),
        P("seq", None, "dp"),
        P(),
    )
    return jax.shard_map(
        body,
        mesh=mesh,
        in_specs=placed,
        out_specs=P(None, None, "seq", None, "dp"),
        check_vma=False,
    )
```

```python
import functools
import math

import jax
import jax.numpy as jnp
from jax import lax
from jax.experimental import pallas as pl
from jax.experimental.pallas import tpu as pltpu
from jax.sharding import PartitionSpec as P

DIM = 5120
HEAD = 128
Q_HEADS = 40
KV_HEADS = 8
MESH = pl.DeviceIdType.MESH


def gelu(z):
    half = 0.5 * z
    return half + half * jnp.tanh(z * (0.7978845608028654 + 0.035677408136300125 * (z * z)))


def flipped(t, mask, bits):
    for bit in bits:
        if mask & bit:
            t = t + bit - 2 * bit * ((t // bit) % 2)
    return t


def window_kernel(
    sizes,
    query_ref,
    keyval_ref,
    in_ref,
    action_ref,
    scale_ref,
    tiles_ref,
    place_ref,
    table_ref,
    taps_ref,
    gains_ref,
    point_hbm,
    ids_ref,
    order_ref,
    out_ref,
    w_all,
    in_all,
    aux_all,
    lat_all,
    embeds,
    squares,
    mixed,
    keys,
    values,
    halos,
    middle,
    conv,
    latent_ref,
    rough,
    start_ref,
    point_ref,
    aux_ref,
    kv_pack,
    place_row,
    ids_row,
    h_send,
    h_recv,
    w_send,
    w_recv,
    i_send,
    i_recv,
    l_send,
    l_recv,
    a_send,
    a_recv,
    o_send,
    o_recv,
    own_sem,
    zi_send,
    zl_send,
):
    D, C, T, edges = sizes
    d = lax.axis_index("dp")
    seq = lax.axis_index("seq")
    c = seq // T
    t = seq % T
    bits = []
    bit = T // 2
    while bit:
        bits.append(bit)
        bit //= 2
    early, last = bits[:-1], bits[-1]
    near_masks = [m for m in range(T) if not m & last]
    near_masks.sort(key=lambda m: m.bit_count())
    depth = query_ref.shape[0]
    in_rows, in_cols = in_ref.shape
    tokens = latent_ref.shape[0]
    rows = D * tokens
    banks = min(C, 2)
    bank = C // banks
    bank_rows = bank * rows
    far = (banks - 1) - c // bank
    near = c // bank
    group = Q_HEADS // KV_HEADS
    qcols = group * HEAD

    orders = [
        sorted(range(C), key=lambda o, i=i: (abs(o - i), o if 2 * i < C else -o)) for i in range(C)
    ]

    def nearest(h):
        value = orders[0][h]
        for i in range(1, C):
            value = jnp.where(c == i, orders[i][h], value)
        return value

    origins = [c] + [nearest(h) for h in range(1, C)]

    def to_c(shift):
        return (d, ((c + shift) % C) * T + t)

    def to_t(bit):
        return (d, c * T + flipped(t, bit, bits))

    def to_d(shift):
        return ((d + shift) % D, seq)

    peers = [to_c(s) for s in range(1, C)] + [to_t(b) for b in bits] + [to_d(s) for s in range(1, D)]
    S = C * T
    above, below = (d, (seq + S - 1) % S), (d, (seq + 1) % S)
    peers += [above, below]
    own = [
        pltpu.make_async_copy(point_hbm, point_ref, own_sem.at[4]),
        pltpu.make_async_copy(
            in_ref,
            in_all.at[
                pl.ds(pl.multiple_of(seq * in_rows, in_rows), in_rows),
                pl.ds(pl.multiple_of(d * in_cols, HEAD), in_cols),
            ],
            own_sem.at[1],
        ),
        pltpu.make_async_copy(
            query_ref.at[:, pl.ds(pl.multiple_of(c * qcols, HEAD), qcols)],
            w_all.at[pl.ds(pl.multiple_of(seq * depth, depth), depth), pl.ds(2 * HEAD, qcols)],
            own_sem.at[0],
        ),
    ]
    point_copy = own.pop(0)
    point_copy.start()
    for copy in own:
        copy.start()
    height, breadth, frames, channels = start_ref.shape
    with jax.named_scope("place"):
        positions = table_ref.shape[0]
        for r in range(height):
            for w in range(breadth):
                base = (r * breadth + w) * frames
                place_row[:, base : base + frames] = place_ref[0, r, w : w + 1, :]
        for k in range(D):
            ids_row[:, k * frames : (k + 1) * frames] = ids_ref[k : k + 1, :]
        chosen = place_row[...] == lax.broadcasted_iota(jnp.int32, (positions, tokens), 0)
        placed = lax.dot_general(
            jnp.where(chosen, 1.0, 0.0).astype(jnp.bfloat16),
            table_ref[...],
            (((0,), (0,)), ((), ())),
            preferred_element_type=jnp.float32,
        )
        for r in range(height):
            for w in range(breadth):
                base = (r * breadth + w) * frames
                tile = tiles_ref[0, :, r, w, :].astype(jnp.float32)
                start_ref[r, w] = (tile + placed[base : base + frames]).astype(jnp.bfloat16)
        actions = action_ref.shape[0]
        aux_ref[:actions] = action_ref[...]
        for k in range(in_cols // HEAD):
            aux_ref[actions:, k * HEAD : (k + 1) * HEAD] = jnp.broadcast_to(
                scale_ref[k : k + 1, :], (16 - actions, HEAD)
            )

    with jax.named_scope("barrier"):
        barrier = pltpu.get_barrier_semaphore()
        for peer in peers:
            pl.semaphore_signal(barrier, inc=1, device_id=peer, device_id_type=MESH)
        pl.semaphore_wait(barrier, len(peers))

    log = []
    waiting = []

    def run(guard, event, *args):
        if not waiting:
            log.append((guard, event, args))
        if guard is None:
            event(*args)
        else:
            pl.when(guard)(functools.partial(event, *args))

    def push(src, dst, send_sem, recv_sem, peer):
        copy = pltpu.make_async_remote_copy(
            src_ref=src,
            dst_ref=dst,
            send_sem=send_sem,
            recv_sem=recv_sem,
            device_id=peer,
            device_id_type=MESH,
        )
        if waiting:
            copy.wait_send()
        else:
            copy.start()

    def arrived(ref, sem):
        if not waiting:
            pltpu.make_async_copy(ref, ref, sem).wait()

    w_cols = [(first, last_col - first) for first, last_col in zip(edges, edges[1:])]
    stages = len(w_cols)
    pieces = [(0, 0, 2 * HEAD)]
    pieces += [(g, max(first, 2 * HEAD), min(count, first + count - 2 * HEAD)) for g, (first, count) in enumerate(w_cols)]

    def w_slot(o, m, piece):
        g, first, count = piece
        origin = o * T + flipped(t, m, bits)
        return w_all.at[
            pl.ds(pl.multiple_of(origin * depth, depth), depth), pl.ds(first, count)
        ]

    def w_own(target, piece):
        g, first, count = piece
        if first == 0:
            return kv_pack.at[target]
        column = target * qcols + first - 2 * HEAD
        return query_ref.at[:, pl.ds(pl.multiple_of(column, HEAD), count)]

    split = in_rows // 2
    WHOLE, HEAD_PART, TAIL_PART = 0, 1, 2

    def part_rows(part):
        return ((0, in_rows), (0, split), (split, in_rows - split))[part]

    def i_slot(o, m, e, part):
        first, count = part_rows(part)
        origin = o * T + flipped(t, m, bits)
        column = ((d + D - e) % D) * in_cols
        return in_all.at[
            pl.ds(pl.multiple_of(origin * in_rows + first, math.gcd(in_rows, split)), count),
            pl.ds(pl.multiple_of(column, HEAD), in_cols),
        ]

    def l_slot(o, e):
        row = ((d + D - e) % D) * tokens
        return lat_all.at[pl.ds(pl.multiple_of(o * rows + row, tokens), tokens)]

    def a_slot(e):
        column = ((d + D - e) % D) * in_cols
        return aux_all.at[:, pl.ds(pl.multiple_of(column, HEAD), in_cols)]

    hops = [(k, way) for k in range(1, C) for way in (1, -1)]

    def hop_origin(k, way):
        return c - way * k

    def hop_guard(k, way):
        return c >= k if way > 0 else c + k < C

    def onward(way):
        return (d, (c + way) * T + t), (c + 1 < C if way > 0 else c >= 1)

    def z_own(src, dst, send_sems, recv_sem):
        for k, way in enumerate((1, -1)):
            if C > 1:
                peer, guard = onward(way)
                pl.when(guard)(functools.partial(push, src, dst, send_sems.at[k], recv_sem, peer))

    def z_hop(slot, send_sem, recv_sem, way):
        peer, guard = onward(way)
        pl.when(guard)(functools.partial(push, slot, slot, send_sem, recv_sem, peer))

    def w_forward(o, m, piece, src):
        k = pieces.index(piece)
        low = -1
        for b in bits:
            if m & b:
                low = bits.index(b)
        for b in bits[low + 1 :]:
            push(src, w_slot(o, m, piece), w_send.at[o, m | b, k], w_recv.at[o, m | b, k], to_t(b))

    def w_across(h, piece):
        k = pieces.index(piece)
        target = origins[h]
        push(
            w_own(target, piece),
            w_slot(c, 0, piece),
            w_send.at[target, 0, k],
            w_recv.at[c, 0, k],
            (d, target * T + t),
        )

    def i_push(o, m, e, part, own, new_m, new_e, peer):
        first, count = part_rows(part)
        src = in_ref.at[pl.ds(first, count)] if own else i_slot(o, m, e, part)
        k = int(part == TAIL_PART)
        push(src, i_slot(o, m, e, part), i_send.at[o, new_m, new_e, k], i_recv.at[o, new_m, new_e, k], peer)

    def i_forward(o, m, e, part, own=False):
        if m & last:
            return
        low = -1
        for b in early:
            if m & b:
                low = early.index(b)
        later = early[low + 1 :]
        if e == 0:
            for b in later:
                i_push(o, m, e, WHOLE, own, m | b, e, to_t(b))
            for shift in range(1, D):
                i_push(o, m, e, HEAD_PART if m else WHOLE, own, m, shift, to_d(shift))
        elif m == 0 or part == TAIL_PART:
            for b in later:
                i_push(o, m, e, TAIL_PART, own, m | b, e, to_t(b))
        i_push(o, m, e, part, own, m | last, e, to_t(last))

    def l_forward(o, src):
        for e in range(1, D):
            push(src, l_slot(o, 0), l_send.at[o, e], l_recv.at[o, e], to_d(e))

    def share_rows(l, source):
        push(source.at[height - 1], halos.at[l, 0], h_send.at[l, 0], h_recv.at[l, 0], below)
        push(source.at[0], halos.at[l, 1], h_send.at[l, 1], h_recv.at[l, 1], above)

    def start_own():
        z_own(in_ref, i_slot(c, 0, 0, WHOLE), zi_send, i_recv.at[c, 0, 0, 0])
        i_forward(c, 0, 0, WHOLE, True)
        for shift in range(1, D):
            push(aux_ref, a_slot(0), a_send.at[shift], a_recv.at[shift], to_d(shift))

    own.append(pltpu.make_async_copy(aux_ref, a_slot(0), own_sem.at[3]))
    own[-1].start()
    run(None, share_rows, 0, start_ref)
    run(None, start_own)

    def i_event(o, m, e, part=0):
        arrived(i_slot(o, m, e, part), i_recv.at[o, m, e, int(part == TAIL_PART)])
        i_forward(o, m, e, part)

    def iz_event(k, way):
        o = hop_origin(k, way)
        slot = i_slot(o, 0, 0, WHOLE)
        arrived(slot, i_recv.at[o, 0, 0, 0])
        z_hop(slot, zi_send.at[2 * k + (way > 0)], i_recv.at[o, 0, 0, 0], way)
        i_forward(o, 0, 0, WHOLE)

    def lz_event(k, way):
        o = hop_origin(k, way)
        slot = l_slot(o, 0)
        arrived(slot, l_recv.at[o, 0])
        z_hop(slot, zl_send.at[2 * k + (way > 0)], l_recv.at[o, 0], way)
        l_forward(o, slot)

    def local_event(k, way):
        o = hop_origin(k, way)
        for m in near_masks:
            if m:
                i_event(o, m, 0)
        for e in range(1, D):
            i_event(o, 0, e)

    def both_ways(event, k):
        with jax.named_scope("%s%d" % (event.__name__[:2], k)):
            for way in (1, -1) if 0 < k < C else ():
                run(hop_guard(k, way), event, k, way)

    def w_event(h, m, piece):
        o = origins[h]
        slot = w_slot(o, m, piece)
        arrived(slot, w_recv.at[o, m, pieces.index(piece)])
        w_forward(o, m, piece, slot)

    def w_forward_own(piece):
        w_forward(c, 0, piece, w_own(c, piece))

    w_pushes = []
    for piece in pieces:
        w_pushes += [(h, piece) for h in range(C - 1, -1, -1)]

    def w_start(count):
        for h, piece in w_pushes[:count]:
            if h:
                run(None, w_across, h, piece)
            else:
                run(None, w_forward_own, piece)
        del w_pushes[:count]

    lanes = 256

    def encode(l, source):
        arrived(halos.at[l, 0], h_recv.at[l, 0])
        arrived(halos.at[l, 1], h_recv.at[l, 1])
        frame_ids = lax.broadcasted_iota(jnp.int32, (frames, lanes), 0)

        def lane_step(j, carry):
            cols = pl.ds(pl.multiple_of(j * lanes, lanes), lanes)
            taps = [taps_ref[k, l : l + 1, cols].astype(jnp.float32) for k in range(27)]

            def patch(r, w):
                if r < 0:
                    return jnp.where(seq > 0, halos[l, 0, w, :, cols].astype(jnp.float32), 0.0)
                if r == height:
                    return jnp.where(seq < S - 1, halos[l, 1, w, :, cols].astype(jnp.float32), 0.0)
                return source[r, w, :, cols].astype(jnp.float32)

            for r in range(height):
                for w in range(breadth):
                    sums = [None] * 3
                    for b in range(3):
                        for k in range(3):
                            if not 0 <= w + k - 1 < breadth:
                                continue
                            value = patch(r + b - 1, w + k - 1)
                            for a in range(3):
                                tap = 9 * a + 3 * b + k
                                term = value * taps[tap]
                                sums[a] = term if sums[a] is None else sums[a] + term
                    total = sums[2]
                    for a in range(2):
                        moved = pltpu.roll(sums[a], 2 - a, 0)
                        total = total + jnp.where(frame_ids >= 2 - a, moved, 0.0)
                    base = (r * breadth + w) * frames
                    conv[base : base + frames, cols] = total
            return carry

        lax.fori_loop(0, channels // lanes, lane_step, 0)
        summed = conv[...]
        factor = lax.rsqrt(jnp.mean(summed * summed, axis=-1, keepdims=True) + 1e-05)
        gain = gains_ref[l].astype(jnp.float32)
        normed = (summed * factor * gain[None]).astype(jnp.bfloat16)
        projected = jnp.dot(normed, point_ref[l], preferred_element_type=jnp.float32)
        change = gelu(projected)
        for r in range(height):
            for w in range(breadth):
                base = (r * breadth + w) * frames
                value = source[r, w].astype(jnp.float32) + change[base : base + frames]
                value = value.astype(jnp.bfloat16)
                if l + 1 < point_ref.shape[0]:
                    middle[l, r, w] = value
                else:
                    rough[base : base + frames] = value

    point_copy.wait()
    source = start_ref
    for l in range(point_ref.shape[0]):
        with jax.named_scope("encode"):
            encode(l, source)
        if l + 1 < point_ref.shape[0]:
            source = middle.at[l]
            run(None, share_rows, l + 1, source)
        if l == 0:
            with jax.named_scope("kv"):
                for o in range(C):
                    for k in range(2):
                        kv_pack[o, :, k * HEAD : (k + 1) * HEAD] = keyval_ref[
                            :, k, o * HEAD : (o + 1) * HEAD
                        ]
            own.append(
                pltpu.make_async_copy(kv_pack.at[c], w_slot(c, 0, pieces[0]), own_sem.at[5])
            )
            own[-1].start()
            both_ways(iz_event, 1)

    with jax.named_scope("order"):
        row_ids = lax.broadcasted_iota(jnp.int32, (tokens, tokens), 0)
        col_ids = lax.broadcasted_iota(jnp.int32, (tokens, tokens), 1)
        cells = tokens // frames
        row_cells = row_ids % cells
        wanted = row_cells // breadth * breadth
        for w in range(breadth):
            wanted = wanted + jnp.where(row_cells % breadth == w, order_ref[w], 0)
        moved = (wanted == col_ids // frames) & (row_ids // cells == col_ids % frames)
        latent_ref[...] = jnp.dot(
            jnp.where(moved, 1.0, 0.0).astype(jnp.bfloat16), rough[...], preferred_element_type=jnp.float32
        ).astype(jnp.bfloat16)

    def start_latent():
        z_own(latent_ref, l_slot(c, 0), zl_send, l_recv.at[c, 0])
        l_forward(c, latent_ref)

    run(None, start_latent)
    run(None, local_event, 0, 1)
    latent_copy = pltpu.make_async_copy(latent_ref, l_slot(c, 0), own_sem.at[2])
    latent_copy.start()
    own.append(latent_copy)

    def w_events(piece, count):
        with jax.named_scope("w%d_%d" % (pieces.index(piece), count)):
            for m in range(T):
                if (m & ~last).bit_count() + (T if m & last else 0) == count:
                    for h in range(C - 1, -1, -1):
                        if h or m:
                            run(None, w_event, h, m, piece)

    both_ways(iz_event, 2)
    both_ways(local_event, 1)
    both_ways(lz_event, 1)
    both_ways(iz_event, 3)
    both_ways(lz_event, 2)
    w_start(2)
    both_ways(local_event, 2)
    w_start(2)
    both_ways(lz_event, 3)
    w_start(4)
    both_ways(local_event, 3)
    for k in range(4, C):
        for event in (iz_event, local_event, lz_event):
            both_ways(event, k)
    w_start(len(w_pushes))
    steps = len(early) + 1
    w_todo = [(k + 2.5 * count, k, count) for k in range(len(pieces)) for count in range(steps)]
    w_todo = [(pieces[k], count) for _, k, count in sorted(w_todo)]

    def core_events(e):
        with jax.named_scope("core"):
            for h in range(C):
                for m in near_masks:
                    if m and e:
                        run(None, i_event, origins[h], m | last, e, HEAD_PART)
                        run(None, i_event, origins[h], m | last, e, TAIL_PART)
                    else:
                        run(None, i_event, origins[h], m | last, e)

    def cross_events(e):
        with jax.named_scope("cross"):
            for h in range(C):
                for m in near_masks:
                    if m:
                        run(None, i_event, origins[h], m, e, HEAD_PART)
                        run(None, i_event, origins[h], m, e, TAIL_PART)

    chunk = in_cols // 2 if in_cols % (2 * HEAD) == 0 else in_cols
    chosen = ids_row[...] == lax.broadcasted_iota(jnp.int32, (16, D * frames), 0)
    picked = jnp.where(chosen, 1.0, 0.0).astype(jnp.bfloat16)

    def rows_of(which):
        return pl.ds(pl.multiple_of(which * bank_rows, bank_rows), bank_rows)

    def embed_bank(which, e):
        at = rows_of(which)
        first = ((d + D - e) % D) * in_cols
        if e == 0:
            squares[at] = jnp.zeros((bank_rows, HEAD), jnp.float32)

        def step(j, carry):
            cols = pl.ds(pl.multiple_of(first + j * chunk, HEAD), chunk)
            z = jnp.dot(lat_all[at], in_all[:, cols], preferred_element_type=jnp.float32)
            action = lax.dot_general(
                picked,
                aux_all[:, cols],
                (((0,), (0,)), ((), ())),
                preferred_element_type=jnp.float32,
            )
            action = jnp.broadcast_to(
                action.reshape(1, D, frames, 1, chunk),
                (bank, D, frames, cells, chunk),
            )
            g = gelu(z + action.reshape(bank_rows, chunk))
            gain = aux_all[:, cols].astype(jnp.float32)[8:9]
            embeds[at, cols] = (g * gain).astype(jnp.bfloat16)
            square = g * g
            part = square[:, :HEAD]
            for k in range(1, chunk // HEAD):
                part = part + square[:, k * HEAD : (k + 1) * HEAD]
            squares[at] += part
            return carry

        with jax.named_scope("embed"):
            lax.fori_loop(0, in_cols // chunk, step, 0)

    def take_w(count):
        for item in w_todo[:count]:
            w_events(*item)
        del w_todo[:count]

    core_events(0)
    for copy in own:
        copy.wait()

    def lat_bank(inside):
        with jax.named_scope("lx"):
            for h in range(bank) if inside else range(bank, C):
                for k in range(1, D):
                    arrived(l_slot(origins[h], k), l_recv.at[origins[h], k])

    if banks > 1:
        lat_bank(True)
        embed_bank(near, 0)
    take_w(1)
    lat_bank(False) if banks > 1 else lat_bank(True)
    embed_bank(far, 0)
    take_w(1)
    for e in range(1, D):
        cross_events(e)
        with jax.named_scope("aux"):
            arrived(a_slot(e), a_recv.at[e])
        core_events(e)
        embed_bank(far, e)
    take_w(3)

    def need_w(g):
        with jax.named_scope("need"):
            while any(piece[0] <= g for piece, count in w_todo):
                take_w(1)
            for piece in pieces:
                if piece[0] == g:
                    for count in range(T, T + steps):
                        w_events(piece, count)

    seen = (row_ids % cells == col_ids % cells) & (row_ids >= col_ids)

    pair = jnp.where(
        lax.broadcasted_iota(jnp.int32, (2 * HEAD, 2 * HEAD), 0) // HEAD
        == lax.broadcasted_iota(jnp.int32, (2 * HEAD, 2 * HEAD), 1) // HEAD,
        1.0,
        0.0,
    ).astype(jnp.bfloat16)

    def unit(x):
        width = x.shape[1]
        total = jnp.dot(
            (x * x).astype(jnp.bfloat16), pair[:width, :width], preferred_element_type=jnp.float32
        )
        return x * lax.rsqrt(total * (1.0 / HEAD) + 1e-06)

    def mix_bank(which, g):
        first, count = w_cols[g]
        base = which * bank_rows
        at = rows_of(which)
        total = jnp.dot(
            embeds[at], w_all[:, first : first + count], preferred_element_type=jnp.float32
        )
        mean = jnp.sum(squares[at], axis=-1, keepdims=True) / DIM
        total = total * lax.rsqrt(mean + 1e-05)
        if g == 0:
            keys[at] = unit(total[:, :HEAD]).astype(jnp.bfloat16)
            values[at, :HEAD] = total[:, HEAD : 2 * HEAD].astype(jnp.bfloat16)
            values[at, HEAD:] = jnp.ones((bank_rows, HEAD), jnp.bfloat16)
        key, value = keys[at], values[at]
        left = 2 * HEAD if g == 0 else 0
        while left < count:
            width = min(2 * HEAD, count - left)
            query = (unit(total[:, left : left + width]) * HEAD**-0.5).astype(jnp.bfloat16)
            for inner in range(0, width, HEAD):
                to = first + left + inner - 2 * HEAD
                spans = [slice(i, i + tokens) for i in range(0, bank_rows, tokens)]
                scores = [
                    lax.dot_general(
                        query[span, inner : inner + HEAD],
                        key[span],
                        (((1,), (1,)), ((), ())),
                        preferred_element_type=jnp.float32,
                    )
                    for span in spans
                ]
                raised = [
                    jnp.where(seen, jnp.exp(score), 0.0).astype(jnp.bfloat16) for score in scores
                ]
                for i, span in enumerate(spans):
                    both = jnp.dot(raised[i], value[span], preferred_element_type=jnp.float32)
                    result = (both[:, :HEAD] / both[:, HEAD:]).astype(jnp.bfloat16)
                    mixed[pl.ds(pl.multiple_of(base + i * tokens, tokens), tokens), to : to + HEAD] = result
            left += width

    def out_cols(g):
        first, count = w_cols[g]
        return (0, count - 2 * HEAD) if g == 0 else (first - 2 * HEAD, count)

    def block_rows(where):
        return pl.ds(pl.multiple_of(where * rows, rows), rows)

    def send_of(where, g):
        first, count = out_cols(g)
        return pltpu.make_async_remote_copy(
            src_ref=mixed.at[block_rows(where), pl.ds(first, count)],
            dst_ref=out_ref.at[:, pl.ds(pl.multiple_of(c * qcols + first, HEAD), count)],
            send_sem=o_send.at[where, g],
            recv_sem=o_recv.at[c, g],
            device_id=(d, where * T + t),
            device_id_type=MESH,
        )

    far_blocks = [far * bank + j for j in range(bank)] if banks > 1 else []
    near_blocks = [near * bank + (c + j) % bank for j in range(1, bank)]

    for g in range(stages):
        need_w(g)
        for which, blocks in ((far, far_blocks), (near, near_blocks))[2 - banks :]:
            with jax.named_scope("mix"):
                mix_bank(which, g)
            for where in blocks:
                send_of(where, g).start()
            if g == 0 and blocks is far_blocks:
                for e in range(1, D):
                    embed_bank(near, e)
    keep = pltpu.make_async_copy(
        mixed.at[block_rows(c)],
        out_ref.at[:, pl.ds(pl.multiple_of(c * qcols, HEAD), qcols)],
        own_sem.at[0],
    )
    keep.start()
    with jax.named_scope("tail"):
        for g in range(stages):
            first, count = out_cols(g)
            for where in near_blocks + far_blocks:
                send_of(where, g).wait_send()
                column = where * qcols + first
                arrived(
                    out_ref.at[:, pl.ds(pl.multiple_of(column, HEAD), count)], o_recv.at[where, g]
                )
        keep.wait()
    waiting.append(True)
    for guard, event, args in log:
        run(guard, event, *args)


def body(
    tiles,
    patch_index,
    pos_table,
    depth_kernel,
    enc_gain,
    point_weight,
    action_ids,
    w_in,
    action_table,
    dyn_gain,
    w_query,
    w_keyval,
    seq_order,
):
    clip_local, frames, height, breadth, channels = tiles.shape
    positions = pos_table.shape[0]
    blocks = depth_kernel.shape[0]
    D, S = lax.axis_size("dp"), lax.axis_size("seq")
    kv_local = w_keyval.shape[2] // HEAD
    C = math.gcd(kv_local, S)
    T = S // C
    assert T & (T - 1) == 0 and T > 1 and clip_local == 1 and kv_local == C
    group = Q_HEADS // KV_HEADS
    depth = w_query.shape[0]

    cells = height * breadth
    tokens = frames * cells
    assert action_table.shape[0] == 8 and depth_kernel.shape[1] == 27
    width = (2 + group) * HEAD
    qcols = group * HEAD
    bf16, f32 = jnp.bfloat16, jnp.float32
    dma = pltpu.SemaphoreType.DMA
    out = pl.pallas_call(
        functools.partial(window_kernel, (D, C, T, [x * HEAD for x in (0, 2 + group // 2, 1 + group, 2 + group)])),
        out_shape=jax.ShapeDtypeStruct((D * tokens, C * qcols), bf16),
        in_specs=[
            pl.BlockSpec(memory_space=space)
            for space in [pl.ANY, pltpu.VMEM, pl.ANY]
            + [pltpu.VMEM] * 7
            + [pl.ANY, pltpu.VMEM, pltpu.SMEM]
        ],
        out_specs=pl.BlockSpec(memory_space=pltpu.VMEM),
        scratch_shapes=[
            pltpu.VMEM((S * depth, width), bf16),
            pltpu.VMEM((channels, DIM), bf16),
            pltpu.VMEM((16, DIM), bf16),
            pltpu.VMEM((C * D * tokens, channels), bf16),
            pltpu.VMEM((C * D * tokens, DIM), bf16),
            pltpu.VMEM((C * D * tokens, HEAD), f32),
            pltpu.VMEM((C * D * tokens, qcols), bf16),
            pltpu.VMEM((C * D * tokens, HEAD), bf16),
            pltpu.VMEM((C * D * tokens, 2 * HEAD), bf16),
            pltpu.VMEM((blocks, 2, breadth, frames, channels), bf16),
            pltpu.VMEM((max(blocks - 1, 1), height, breadth, frames, channels), bf16),
            pltpu.VMEM((tokens, channels), f32),
            pltpu.VMEM((tokens, channels), bf16),
            pltpu.VMEM((tokens, channels), bf16),
            pltpu.VMEM((height, breadth, frames, channels), bf16),
            pltpu.VMEM(point_weight.shape, bf16),
            pltpu.VMEM((16, w_in.shape[1]), bf16),
            pltpu.VMEM((C, depth, 2 * HEAD), bf16),
            pltpu.VMEM((1, tokens), jnp.int32),
            pltpu.VMEM((1, D * frames), jnp.int32),
            dma((blocks, 2)),
            dma((blocks, 2)),
            dma((C, T, 4)),
            dma((C, T, 4)),
            dma((C, T, D, 2)),
            dma((C, T, D, 2)),
            dma((C, D)),
            dma((C, D)),
            dma((D,)),
            dma((D,)),
            dma((C, 3)),
            dma((C, 3)),
            dma((6,)),
            dma((2 * C,)),
            dma((2 * C,)),
        ],
        compiler_params=pltpu.CompilerParams(
            collective_id=0, has_side_effects=True, vmem_limit_bytes=60 * 1024 * 1024
        ),
    )(
        w_query,
        w_keyval,
        w_in,
        action_table,
        dyn_gain.reshape(-1, HEAD),
        tiles,
        patch_index.transpose(0, 2, 3, 1),
        pos_table,
        depth_kernel.transpose(1, 0, 2),
        enc_gain,
        point_weight,
        action_ids,
        seq_order,
    )
    return out.reshape(D, frames, height, breadth, -1)


def solution(mesh):
    placed = (
        P("dp", None, "seq", None, None),
        P("dp", None, "seq", None),
        P(),
        P(),
        P(),
        P(),
        P(),
        P("seq", "dp"),
        P(None, "dp"),
        P("dp"),
        P("seq", "dp"),
        P("seq", None, "dp"),
        P(),
    )
    return jax.shard_map(
        body,
        mesh=mesh,
        in_specs=placed,
        out_specs=P(None, None, "seq", None, "dp"),
        check_vma=False,
    )
```

```python
import functools
import math

import jax
import jax.numpy as jnp
from jax import lax
from jax.experimental import pallas as pl
from jax.experimental.pallas import tpu as pltpu
from jax.sharding import PartitionSpec as P

DIM = 5120
HEAD = 128
Q_HEADS = 40
KV_HEADS = 8
MESH = pl.DeviceIdType.MESH


def gelu(z):
    half = 0.5 * z
    return half + half * jnp.tanh(z * (0.7978845608028654 + 0.035677408136300125 * (z * z)))


def flipped(t, mask, bits):
    for bit in bits:
        if mask & bit:
            t = t + bit - 2 * bit * ((t // bit) % 2)
    return t


def window_kernel(
    sizes,
    query_ref,
    keyval_ref,
    in_ref,
    action_ref,
    scale_ref,
    tiles_ref,
    place_ref,
    table_ref,
    taps_ref,
    gains_ref,
    point_hbm,
    ids_ref,
    order_ref,
    out_ref,
    w_all,
    in_all,
    aux_all,
    lat_all,
    embeds,
    squares,
    mixed,
    keys,
    values,
    halos,
    middle,
    conv,
    latent_ref,
    rough,
    start_ref,
    point_ref,
    aux_ref,
    kv_pack,
    place_row,
    ids_row,
    h_send,
    h_recv,
    w_send,
    w_recv,
    i_send,
    i_recv,
    l_send,
    l_recv,
    a_send,
    a_recv,
    o_send,
    o_recv,
    own_sem,
    zi_send,
    zl_send,
):
    D, C, T, edges = sizes
    d = lax.axis_index("dp")
    seq = lax.axis_index("seq")
    c = seq // T
    t = seq % T
    bits = []
    bit = T // 2
    while bit:
        bits.append(bit)
        bit //= 2
    early, last = bits[:-1], bits[-1]
    near_masks = [m for m in range(T) if not m & last]
    near_masks.sort(key=lambda m: m.bit_count())
    depth = query_ref.shape[0]
    in_rows, in_cols = in_ref.shape
    tokens = latent_ref.shape[0]
    rows = D * tokens
    banks = min(C, 2)
    bank = C // banks
    bank_rows = bank * rows
    far = (banks - 1) - c // bank
    near = c // bank
    group = Q_HEADS // KV_HEADS
    qcols = group * HEAD

    orders = [
        sorted(range(C), key=lambda o, i=i: (abs(o - i), o if 2 * i < C else -o)) for i in range(C)
    ]

    def nearest(h):
        value = orders[0][h]
        for i in range(1, C):
            value = jnp.where(c == i, orders[i][h], value)
        return value

    origins = [c] + [nearest(h) for h in range(1, C)]

    def to_c(shift):
        return (d, ((c + shift) % C) * T + t)

    def to_t(bit):
        return (d, c * T + flipped(t, bit, bits))

    def to_d(shift):
        return ((d + shift) % D, seq)

    peers = [to_c(s) for s in range(1, C)] + [to_t(b) for b in bits] + [to_d(s) for s in range(1, D)]
    S = C * T
    above, below = (d, (seq + S - 1) % S), (d, (seq + 1) % S)
    peers += [above, below]
    own = [
        pltpu.make_async_copy(point_hbm, point_ref, own_sem.at[4]),
        pltpu.make_async_copy(
            in_ref,
            in_all.at[
                pl.ds(pl.multiple_of(seq * in_rows, in_rows), in_rows),
                pl.ds(pl.multiple_of(d * in_cols, HEAD), in_cols),
            ],
            own_sem.at[1],
        ),
        pltpu.make_async_copy(
            query_ref.at[:, pl.ds(pl.multiple_of(c * qcols, HEAD), qcols)],
            w_all.at[pl.ds(pl.multiple_of(seq * depth, depth), depth), pl.ds(2 * HEAD, qcols)],
            own_sem.at[0],
        ),
    ]
    point_copy = own.pop(0)
    point_copy.start()
    for copy in own:
        copy.start()
    height, breadth, frames, channels = start_ref.shape
    with jax.named_scope("place"):
        positions = table_ref.shape[0]
        for r in range(height):
            for w in range(breadth):
                base = (r * breadth + w) * frames
                place_row[:, base : base + frames] = place_ref[0, r, w : w + 1, :]
        for k in range(D):
            ids_row[:, k * frames : (k + 1) * frames] = ids_ref[k : k + 1, :]
        chosen = place_row[...] == lax.broadcasted_iota(jnp.int32, (positions, tokens), 0)
        placed = lax.dot_general(
            jnp.where(chosen, 1.0, 0.0).astype(jnp.bfloat16),
            table_ref[...],
            (((0,), (0,)), ((), ())),
            preferred_element_type=jnp.float32,
        )
        for r in range(height):
            for w in range(breadth):
                base = (r * breadth + w) * frames
                tile = tiles_ref[0, :, r, w, :].astype(jnp.float32)
                start_ref[r, w] = (tile + placed[base : base + frames]).astype(jnp.bfloat16)
        actions = action_ref.shape[0]
        aux_ref[:actions] = action_ref[...]
        for k in range(in_cols // HEAD):
            aux_ref[actions:, k * HEAD : (k + 1) * HEAD] = jnp.broadcast_to(
                scale_ref[k : k + 1, :], (16 - actions, HEAD)
            )

    with jax.named_scope("barrier"):
        barrier = pltpu.get_barrier_semaphore()
        for peer in peers:
            pl.semaphore_signal(barrier, inc=1, device_id=peer, device_id_type=MESH)
        pl.semaphore_wait(barrier, len(peers))

    log = []
    waiting = []

    def run(guard, event, *args):
        if not waiting:
            log.append((guard, event, args))
        if guard is None:
            event(*args)
        else:
            pl.when(guard)(functools.partial(event, *args))

    def push(src, dst, send_sem, recv_sem, peer):
        copy = pltpu.make_async_remote_copy(
            src_ref=src,
            dst_ref=dst,
            send_sem=send_sem,
            recv_sem=recv_sem,
            device_id=peer,
            device_id_type=MESH,
        )
        if waiting:
            copy.wait_send()
        else:
            copy.start()

    def arrived(ref, sem):
        if not waiting:
            pltpu.make_async_copy(ref, ref, sem).wait()

    w_cols = [(first, last_col - first) for first, last_col in zip(edges, edges[1:])]
    stages = len(w_cols)
    pieces = [(0, 0, 2 * HEAD)]
    pieces += [(g, max(first, 2 * HEAD), min(count, first + count - 2 * HEAD)) for g, (first, count) in enumerate(w_cols)]

    def w_slot(o, m, piece):
        g, first, count = piece
        origin = o * T + flipped(t, m, bits)
        return w_all.at[
            pl.ds(pl.multiple_of(origin * depth, depth), depth), pl.ds(first, count)
        ]

    def w_own(target, piece):
        g, first, count = piece
        if first == 0:
            return kv_pack.at[target]
        column = target * qcols + first - 2 * HEAD
        return query_ref.at[:, pl.ds(pl.multiple_of(column, HEAD), count)]

    split = in_rows // 2
    WHOLE, HEAD_PART, TAIL_PART = 0, 1, 2

    def part_rows(part):
        return ((0, in_rows), (0, split), (split, in_rows - split))[part]

    def i_slot(o, m, e, part):
        first, count = part_rows(part)
        origin = o * T + flipped(t, m, bits)
        column = ((d + D - e) % D) * in_cols
        return in_all.at[
            pl.ds(pl.multiple_of(origin * in_rows + first, math.gcd(in_rows, split)), count),
            pl.ds(pl.multiple_of(column, HEAD), in_cols),
        ]

    def l_slot(o, e):
        row = ((d + D - e) % D) * tokens
        return lat_all.at[pl.ds(pl.multiple_of(o * rows + row, tokens), tokens)]

    def a_slot(e):
        column = ((d + D - e) % D) * in_cols
        return aux_all.at[:, pl.ds(pl.multiple_of(column, HEAD), in_cols)]

    hops = [(k, way) for k in range(1, C) for way in (1, -1)]

    def hop_origin(k, way):
        return c - way * k

    def hop_guard(k, way):
        return c >= k if way > 0 else c + k < C

    def onward(way):
        return (d, (c + way) * T + t), (c + 1 < C if way > 0 else c >= 1)

    def z_own(src, dst, send_sems, recv_sem):
        for k, way in enumerate((1, -1)):
            if C > 1:
                peer, guard = onward(way)
                pl.when(guard)(functools.partial(push, src, dst, send_sems.at[k], recv_sem, peer))

    def z_hop(slot, send_sem, recv_sem, way):
        peer, guard = onward(way)
        pl.when(guard)(functools.partial(push, slot, slot, send_sem, recv_sem, peer))

    def w_forward(o, m, piece, src):
        k = pieces.index(piece)
        low = -1
        for b in bits:
            if m & b:
                low = bits.index(b)
        for b in bits[low + 1 :]:
            push(src, w_slot(o, m, piece), w_send.at[o, m | b, k], w_recv.at[o, m | b, k], to_t(b))

    def w_across(h, piece):
        k = pieces.index(piece)
        target = origins[h]
        push(
            w_own(target, piece),
            w_slot(c, 0, piece),
            w_send.at[target, 0, k],
            w_recv.at[c, 0, k],
            (d, target * T + t),
        )

    def i_push(o, m, e, part, own, new_m, new_e, peer):
        first, count = part_rows(part)
        src = in_ref.at[pl.ds(first, count)] if own else i_slot(o, m, e, part)
        k = int(part == TAIL_PART)
        push(src, i_slot(o, m, e, part), i_send.at[o, new_m, new_e, k], i_recv.at[o, new_m, new_e, k], peer)

    def i_forward(o, m, e, part, own=False):
        if m & last:
            return
        low = -1
        for b in early:
            if m & b:
                low = early.index(b)
        later = early[low + 1 :]
        if e == 0:
            for b in later:
                i_push(o, m, e, WHOLE, own, m | b, e, to_t(b))
            for shift in range(1, D):
                i_push(o, m, e, HEAD_PART if m else WHOLE, own, m, shift, to_d(shift))
        elif m == 0 or part == TAIL_PART:
            for b in later:
                i_push(o, m, e, TAIL_PART, own, m | b, e, to_t(b))
        i_push(o, m, e, part, own, m | last, e, to_t(last))

    def l_forward(o, src):
        for e in range(1, D):
            push(src, l_slot(o, 0), l_send.at[o, e], l_recv.at[o, e], to_d(e))

    def share_rows(l, source):
        push(source.at[height - 1], halos.at[l, 0], h_send.at[l, 0], h_recv.at[l, 0], below)
        push(source.at[0], halos.at[l, 1], h_send.at[l, 1], h_recv.at[l, 1], above)

    def start_own():
        z_own(in_ref, i_slot(c, 0, 0, WHOLE), zi_send, i_recv.at[c, 0, 0, 0])
        i_forward(c, 0, 0, WHOLE, True)
        for shift in range(1, D):
            push(aux_ref, a_slot(0), a_send.at[shift], a_recv.at[shift], to_d(shift))

    own.append(pltpu.make_async_copy(aux_ref, a_slot(0), own_sem.at[3]))
    own[-1].start()
    run(None, share_rows, 0, start_ref)
    run(None, start_own)

    def i_event(o, m, e, part=0):
        arrived(i_slot(o, m, e, part), i_recv.at[o, m, e, int(part == TAIL_PART)])
        i_forward(o, m, e, part)

    def iz_event(k, way):
        o = hop_origin(k, way)
        slot = i_slot(o, 0, 0, WHOLE)
        arrived(slot, i_recv.at[o, 0, 0, 0])
        z_hop(slot, zi_send.at[2 * k + (way > 0)], i_recv.at[o, 0, 0, 0], way)
        i_forward(o, 0, 0, WHOLE)

    def lz_event(k, way):
        o = hop_origin(k, way)
        slot = l_slot(o, 0)
        arrived(slot, l_recv.at[o, 0])
        z_hop(slot, zl_send.at[2 * k + (way > 0)], l_recv.at[o, 0], way)
        l_forward(o, slot)

    def local_event(k, way):
        o = hop_origin(k, way)
        for m in near_masks:
            if m:
                i_event(o, m, 0)
        for e in range(1, D):
            i_event(o, 0, e)

    def both_ways(event, k):
        with jax.named_scope("%s%d" % (event.__name__[:2], k)):
            for way in (1, -1) if 0 < k < C else ():
                run(hop_guard(k, way), event, k, way)

    def w_event(h, m, piece):
        o = origins[h]
        slot = w_slot(o, m, piece)
        arrived(slot, w_recv.at[o, m, pieces.index(piece)])
        w_forward(o, m, piece, slot)

    def w_forward_own(piece):
        w_forward(c, 0, piece, w_own(c, piece))

    w_pushes = []
    for piece in pieces:
        w_pushes += [(h, piece) for h in range(C - 1, -1, -1)]

    def w_start(count):
        for h, piece in w_pushes[:count]:
            if h:
                run(None, w_across, h, piece)
            else:
                run(None, w_forward_own, piece)
        del w_pushes[:count]

    lanes = 256

    def encode(l, source):
        arrived(halos.at[l, 0], h_recv.at[l, 0])
        arrived(halos.at[l, 1], h_recv.at[l, 1])
        frame_ids = lax.broadcasted_iota(jnp.int32, (frames, lanes), 0)

        def lane_step(j, carry):
            cols = pl.ds(pl.multiple_of(j * lanes, lanes), lanes)
            taps = [taps_ref[k, l : l + 1, cols].astype(jnp.float32) for k in range(27)]

            def patch(r, w):
                if r < 0:
                    return jnp.where(seq > 0, halos[l, 0, w, :, cols].astype(jnp.float32), 0.0)
                if r == height:
                    return jnp.where(seq < S - 1, halos[l, 1, w, :, cols].astype(jnp.float32), 0.0)
                return source[r, w, :, cols].astype(jnp.float32)

            for r in range(height):
                for w in range(breadth):
                    sums = [None] * 3
                    for b in range(3):
                        for k in range(3):
                            if not 0 <= w + k - 1 < breadth:
                                continue
                            value = patch(r + b - 1, w + k - 1)
                            for a in range(3):
                                tap = 9 * a + 3 * b + k
                                term = value * taps[tap]
                                sums[a] = term if sums[a] is None else sums[a] + term
                    total = sums[2]
                    for a in range(2):
                        moved = pltpu.roll(sums[a], 2 - a, 0)
                        total = total + jnp.where(frame_ids >= 2 - a, moved, 0.0)
                    base = (r * breadth + w) * frames
                    conv[base : base + frames, cols] = total
            return carry

        lax.fori_loop(0, channels // lanes, lane_step, 0)
        summed = conv[...]
        factor = lax.rsqrt(jnp.mean(summed * summed, axis=-1, keepdims=True) + 1e-05)
        gain = gains_ref[l].astype(jnp.float32)
        normed = (summed * factor * gain[None]).astype(jnp.bfloat16)
        projected = jnp.dot(normed, point_ref[l], preferred_element_type=jnp.float32)
        change = gelu(projected)
        for r in range(height):
            for w in range(breadth):
                base = (r * breadth + w) * frames
                value = source[r, w].astype(jnp.float32) + change[base : base + frames]
                value = value.astype(jnp.bfloat16)
                if l + 1 < point_ref.shape[0]:
                    middle[l, r, w] = value
                else:
                    rough[base : base + frames] = value

    point_copy.wait()
    source = start_ref
    for l in range(point_ref.shape[0]):
        with jax.named_scope("encode"):
            encode(l, source)
        if l + 1 < point_ref.shape[0]:
            source = middle.at[l]
            run(None, share_rows, l + 1, source)
        if l == 0:
            with jax.named_scope("kv"):
                for o in range(C):
                    for k in range(2):
                        kv_pack[o, :, k * HEAD : (k + 1) * HEAD] = keyval_ref[
                            :, k, o * HEAD : (o + 1) * HEAD
                        ]
            own.append(
                pltpu.make_async_copy(kv_pack.at[c], w_slot(c, 0, pieces[0]), own_sem.at[5])
            )
            own[-1].start()
            both_ways(iz_event, 1)

    with jax.named_scope("order"):
        row_ids = lax.broadcasted_iota(jnp.int32, (tokens, tokens), 0)
        col_ids = lax.broadcasted_iota(jnp.int32, (tokens, tokens), 1)
        cells = tokens // frames
        row_cells = row_ids % cells
        wanted = row_cells // breadth * breadth
        for w in range(breadth):
            wanted = wanted + jnp.where(row_cells % breadth == w, order_ref[w], 0)
        moved = (wanted == col_ids // frames) & (row_ids // cells == col_ids % frames)
        latent_ref[...] = jnp.dot(
            jnp.where(moved, 1.0, 0.0).astype(jnp.bfloat16), rough[...], preferred_element_type=jnp.float32
        ).astype(jnp.bfloat16)

    def start_latent():
        z_own(latent_ref, l_slot(c, 0), zl_send, l_recv.at[c, 0])
        l_forward(c, latent_ref)

    run(None, start_latent)
    run(None, local_event, 0, 1)
    latent_copy = pltpu.make_async_copy(latent_ref, l_slot(c, 0), own_sem.at[2])
    latent_copy.start()
    own.append(latent_copy)

    def w_events(piece, count):
        with jax.named_scope("w%d_%d" % (pieces.index(piece), count)):
            for m in range(T):
                if (m & ~last).bit_count() + (T if m & last else 0) == count:
                    for h in range(C - 1, -1, -1):
                        if h or m:
                            run(None, w_event, h, m, piece)

    both_ways(iz_event, 2)
    both_ways(local_event, 1)
    both_ways(lz_event, 1)
    both_ways(iz_event, 3)
    both_ways(lz_event, 2)
    w_start(2)
    both_ways(local_event, 2)
    w_start(2)
    both_ways(lz_event, 3)
    w_start(4)
    both_ways(local_event, 3)
    for k in range(4, C):
        for event in (iz_event, local_event, lz_event):
            both_ways(event, k)
    w_start(len(w_pushes))
    steps = len(early) + 1
    w_todo = [(k + 2 * count, k, count) for k in range(len(pieces)) for count in range(steps)]
    w_todo = [(pieces[k], count) for _, k, count in sorted(w_todo)]

    def core_events(e):
        with jax.named_scope("core"):
            for h in range(C):
                for m in near_masks:
                    if m and e:
                        run(None, i_event, origins[h], m | last, e, HEAD_PART)
                        run(None, i_event, origins[h], m | last, e, TAIL_PART)
                    else:
                        run(None, i_event, origins[h], m | last, e)

    def cross_events(e):
        with jax.named_scope("cross"):
            for h in range(C):
                for m in near_masks:
                    if m:
                        run(None, i_event, origins[h], m, e, HEAD_PART)
                        run(None, i_event, origins[h], m, e, TAIL_PART)

    chunk = in_cols // 2 if in_cols % (2 * HEAD) == 0 else in_cols
    chosen = ids_row[...] == lax.broadcasted_iota(jnp.int32, (16, D * frames), 0)
    picked = jnp.where(chosen, 1.0, 0.0).astype(jnp.bfloat16)

    def rows_of(which):
        return pl.ds(pl.multiple_of(which * bank_rows, bank_rows), bank_rows)

    def embed_bank(which, e):
        at = rows_of(which)
        first = ((d + D - e) % D) * in_cols
        if e == 0:
            squares[at] = jnp.zeros((bank_rows, HEAD), jnp.float32)

        def step(j, carry):
            cols = pl.ds(pl.multiple_of(first + j * chunk, HEAD), chunk)
            z = jnp.dot(lat_all[at], in_all[:, cols], preferred_element_type=jnp.float32)
            action = lax.dot_general(
                picked,
                aux_all[:, cols],
                (((0,), (0,)), ((), ())),
                preferred_element_type=jnp.float32,
            )
            action = jnp.broadcast_to(
                action.reshape(1, D, frames, 1, chunk),
                (bank, D, frames, cells, chunk),
            )
            g = gelu(z + action.reshape(bank_rows, chunk))
            gain = aux_all[:, cols].astype(jnp.float32)[8:9]
            embeds[at, cols] = (g * gain).astype(jnp.bfloat16)
            square = g * g
            part = square[:, :HEAD]
            for k in range(1, chunk // HEAD):
                part = part + square[:, k * HEAD : (k + 1) * HEAD]
            squares[at] += part
            return carry

        with jax.named_scope("embed"):
            lax.fori_loop(0, in_cols // chunk, step, 0)

    def take_w(count):
        for item in w_todo[:count]:
            w_events(*item)
        del w_todo[:count]

    core_events(0)
    for copy in own:
        copy.wait()

    def lat_bank(inside):
        with jax.named_scope("lx"):
            for h in range(bank) if inside else range(bank, C):
                for k in range(1, D):
                    arrived(l_slot(origins[h], k), l_recv.at[origins[h], k])

    if banks > 1:
        lat_bank(True)
        embed_bank(near, 0)
    take_w(1)
    lat_bank(False) if banks > 1 else lat_bank(True)
    embed_bank(far, 0)
    take_w(1)
    for e in range(1, D):
        cross_events(e)
        with jax.named_scope("aux"):
            arrived(a_slot(e), a_recv.at[e])
        core_events(e)
        embed_bank(far, e)
    take_w(2)

    def need_w(g):
        with jax.named_scope("need"):
            while any(piece[0] <= g for piece, count in w_todo):
                take_w(1)
            for piece in pieces:
                if piece[0] == g:
                    for count in range(T, T + steps):
                        w_events(piece, count)

    seen = (row_ids % cells == col_ids % cells) & (row_ids >= col_ids)

    pair = jnp.where(
        lax.broadcasted_iota(jnp.int32, (2 * HEAD, 2 * HEAD), 0) // HEAD
        == lax.broadcasted_iota(jnp.int32, (2 * HEAD, 2 * HEAD), 1) // HEAD,
        1.0,
        0.0,
    ).astype(jnp.bfloat16)

    def unit(x):
        width = x.shape[1]
        total = jnp.dot(
            (x * x).astype(jnp.bfloat16), pair[:width, :width], preferred_element_type=jnp.float32
        )
        return x * lax.rsqrt(total * (1.0 / HEAD) + 1e-06)

    def mix_bank(which, g):
        first, count = w_cols[g]
        base = which * bank_rows
        at = rows_of(which)
        total = jnp.dot(
            embeds[at], w_all[:, first : first + count], preferred_element_type=jnp.float32
        )
        mean = jnp.sum(squares[at], axis=-1, keepdims=True) / DIM
        total = total * lax.rsqrt(mean + 1e-05)
        if g == 0:
            keys[at] = unit(total[:, :HEAD]).astype(jnp.bfloat16)
            values[at, :HEAD] = total[:, HEAD : 2 * HEAD].astype(jnp.bfloat16)
            values[at, HEAD:] = jnp.ones((bank_rows, HEAD), jnp.bfloat16)
        key, value = keys[at], values[at]
        left = 2 * HEAD if g == 0 else 0
        while left < count:
            width = min(2 * HEAD, count - left)
            query = (unit(total[:, left : left + width]) * HEAD**-0.5).astype(jnp.bfloat16)
            for inner in range(0, width, HEAD):
                to = first + left + inner - 2 * HEAD
                spans = [slice(i, i + tokens) for i in range(0, bank_rows, tokens)]
                scores = [
                    lax.dot_general(
                        query[span, inner : inner + HEAD],
                        key[span],
                        (((1,), (1,)), ((), ())),
                        preferred_element_type=jnp.float32,
                    )
                    for span in spans
                ]
                raised = [
                    jnp.where(seen, jnp.exp(score), 0.0).astype(jnp.bfloat16) for score in scores
                ]
                for i, span in enumerate(spans):
                    both = jnp.dot(raised[i], value[span], preferred_element_type=jnp.float32)
                    result = (both[:, :HEAD] / both[:, HEAD:]).astype(jnp.bfloat16)
                    mixed[pl.ds(pl.multiple_of(base + i * tokens, tokens), tokens), to : to + HEAD] = result
            left += width

    def out_cols(g):
        first, count = w_cols[g]
        return (0, count - 2 * HEAD) if g == 0 else (first - 2 * HEAD, count)

    def block_rows(where):
        return pl.ds(pl.multiple_of(where * rows, rows), rows)

    def send_of(where, g):
        first, count = out_cols(g)
        return pltpu.make_async_remote_copy(
            src_ref=mixed.at[block_rows(where), pl.ds(first, count)],
            dst_ref=out_ref.at[:, pl.ds(pl.multiple_of(c * qcols + first, HEAD), count)],
            send_sem=o_send.at[where, g],
            recv_sem=o_recv.at[c, g],
            device_id=(d, where * T + t),
            device_id_type=MESH,
        )

    far_blocks = [far * bank + j for j in range(bank)] if banks > 1 else []
    near_blocks = [near * bank + (c + j) % bank for j in range(1, bank)]

    for g in range(stages):
        need_w(g)
        for which, blocks in ((far, far_blocks), (near, near_blocks))[2 - banks :]:
            with jax.named_scope("mix"):
                mix_bank(which, g)
            for where in blocks:
                send_of(where, g).start()
            if g == 0 and blocks is far_blocks:
                take_w(1)
                for e in range(1, D):
                    embed_bank(near, e)
    keep = pltpu.make_async_copy(
        mixed.at[block_rows(c)],
        out_ref.at[:, pl.ds(pl.multiple_of(c * qcols, HEAD), qcols)],
        own_sem.at[0],
    )
    keep.start()
    with jax.named_scope("tail"):
        for g in range(stages):
            first, count = out_cols(g)
            for where in near_blocks + far_blocks:
                send_of(where, g).wait_send()
                column = where * qcols + first
                arrived(
                    out_ref.at[:, pl.ds(pl.multiple_of(column, HEAD), count)], o_recv.at[where, g]
                )
        keep.wait()
    waiting.append(True)
    for guard, event, args in log:
        run(guard, event, *args)


def body(
    tiles,
    patch_index,
    pos_table,
    depth_kernel,
    enc_gain,
    point_weight,
    action_ids,
    w_in,
    action_table,
    dyn_gain,
    w_query,
    w_keyval,
    seq_order,
):
    clip_local, frames, height, breadth, channels = tiles.shape
    positions = pos_table.shape[0]
    blocks = depth_kernel.shape[0]
    D, S = lax.axis_size("dp"), lax.axis_size("seq")
    kv_local = w_keyval.shape[2] // HEAD
    C = math.gcd(kv_local, S)
    T = S // C
    assert T & (T - 1) == 0 and T > 1 and clip_local == 1 and kv_local == C
    group = Q_HEADS // KV_HEADS
    depth = w_query.shape[0]

    cells = height * breadth
    tokens = frames * cells
    assert action_table.shape[0] == 8 and depth_kernel.shape[1] == 27
    width = (2 + group) * HEAD
    qcols = group * HEAD
    bf16, f32 = jnp.bfloat16, jnp.float32
    dma = pltpu.SemaphoreType.DMA
    out = pl.pallas_call(
        functools.partial(window_kernel, (D, C, T, [x * HEAD for x in (0, 2 + group // 2, 1 + group, 2 + group)])),
        out_shape=jax.ShapeDtypeStruct((D * tokens, C * qcols), bf16),
        in_specs=[
            pl.BlockSpec(memory_space=space)
            for space in [pl.ANY, pltpu.VMEM, pl.ANY]
            + [pltpu.VMEM] * 7
            + [pl.ANY, pltpu.VMEM, pltpu.SMEM]
        ],
        out_specs=pl.BlockSpec(memory_space=pltpu.VMEM),
        scratch_shapes=[
            pltpu.VMEM((S * depth, width), bf16),
            pltpu.VMEM((channels, DIM), bf16),
            pltpu.VMEM((16, DIM), bf16),
            pltpu.VMEM((C * D * tokens, channels), bf16),
            pltpu.VMEM((C * D * tokens, DIM), bf16),
            pltpu.VMEM((C * D * tokens, HEAD), f32),
            pltpu.VMEM((C * D * tokens, qcols), bf16),
            pltpu.VMEM((C * D * tokens, HEAD), bf16),
            pltpu.VMEM((C * D * tokens, 2 * HEAD), bf16),
            pltpu.VMEM((blocks, 2, breadth, frames, channels), bf16),
            pltpu.VMEM((max(blocks - 1, 1), height, breadth, frames, channels), bf16),
            pltpu.VMEM((tokens, channels), f32),
            pltpu.VMEM((tokens, channels), bf16),
            pltpu.VMEM((tokens, channels), bf16),
            pltpu.VMEM((height, breadth, frames, channels), bf16),
            pltpu.VMEM(point_weight.shape, bf16),
            pltpu.VMEM((16, w_in.shape[1]), bf16),
            pltpu.VMEM((C, depth, 2 * HEAD), bf16),
            pltpu.VMEM((1, tokens), jnp.int32),
            pltpu.VMEM((1, D * frames), jnp.int32),
            dma((blocks, 2)),
            dma((blocks, 2)),
            dma((C, T, 4)),
            dma((C, T, 4)),
            dma((C, T, D, 2)),
            dma((C, T, D, 2)),
            dma((C, D)),
            dma((C, D)),
            dma((D,)),
            dma((D,)),
            dma((C, 3)),
            dma((C, 3)),
            dma((6,)),
            dma((2 * C,)),
            dma((2 * C,)),
        ],
        compiler_params=pltpu.CompilerParams(
            collective_id=0, has_side_effects=True, vmem_limit_bytes=60 * 1024 * 1024
        ),
    )(
        w_query,
        w_keyval,
        w_in,
        action_table,
        dyn_gain.reshape(-1, HEAD),
        tiles,
        patch_index.transpose(0, 2, 3, 1),
        pos_table,
        depth_kernel.transpose(1, 0, 2),
        enc_gain,
        point_weight,
        action_ids,
        seq_order,
    )
    return out.reshape(D, frames, height, breadth, -1)


def solution(mesh):
    placed = (
        P("dp", None, "seq", None, None),
        P("dp", None, "seq", None),
        P(),
        P(),
        P(),
        P(),
        P(),
        P("seq", "dp"),
        P(None, "dp"),
        P("dp"),
        P("seq", "dp"),
        P("seq", None, "dp"),
        P(),
    )
    return jax.shard_map(
        body,
        mesh=mesh,
        in_specs=placed,
        out_specs=P(None, None, "seq", None, "dp"),
        check_vma=False,
    )
```
